256 devices in a mesh: rep: 2 (over core), dp: 128 (over x, y, z).
Axes of the slice: x: 4, y: 4, z: 8, core: 2. Of those that a mesh axis runs over, the one named last changes fastest.
Arguments:
- x: bfloat16 [256, 1024, 896], P(('rep', 'dp')), parts along dimension 0
- dy: bfloat16 [256, 1024, 896], P(('rep', 'dp')), parts along dimension 0
- wq: bfloat16 [1, 896, 1024], replicated
- wk: bfloat16 [1, 896, 512], replicated
- wv: bfloat16 [1, 896, 512], replicated
- wo: bfloat16 [1, 1024, 896], replicated
- w_gate: bfloat16 [1, 896, 3584], replicated
- w_up: bfloat16 [1, 896, 3584], replicated
- w_down: bfloat16 [1, 3584, 896], replicated
- m_wq: float32 [1, 896, 1024], replicated
- m_wk: float32 [1, 896, 512], replicated
- m_wv: float32 [1, 896, 512], replicated
- m_wo: float32 [1, 1024, 896], replicated
- m_w_gate: float32 [1, 896, 3584], replicated
- m_w_up: float32 [1, 896, 3584], replicated
- m_w_down: float32 [1, 3584, 896], replicated
- v_wq: float32 [1, 896, 1024], replicated
- v_wk: float32 [1, 896, 512], replicated
- v_wv: float32 [1, 896, 512], replicated
- v_wo: float32 [1, 1024, 896], replicated
- v_w_gate: float32 [1, 896, 3584], replicated
- v_w_up: float32 [1, 896, 3584], replicated
- v_w_down: float32 [1, 3584, 896], replicated
Outputs:
- output 1: bfloat16 [2, 896, 1024], P('rep'), parts along dimension 0
- output 2: bfloat16 [2, 896, 512], P('rep'), parts along dimension 0
- output 3: bfloat16 [2, 896, 512], P('rep'), parts along dimension 0
- output 4: bfloat16 [2, 1024, 896], P('rep'), parts along dimension 0
- output 5: bfloat16 [2, 896, 3584], P('rep'), parts along dimension 0
- output 6: bfloat16 [2, 896, 3584], P('rep'), parts along dimension 0
- output 7: bfloat16 [2, 3584, 896], P('rep'), parts along dimension 0
- output 8: float32 [2, 896, 1024], P('rep'), parts along dimension 0
- output 9: float32 [2, 896, 512], P('rep'), parts along dimension 0
- output 10: float32 [2, 896, 512], P('rep'), parts along dimension 0
- output 11: float32 [2, 1024, 896], P('rep'), parts along dimension 0
- output 12: float32 [2, 896, 3584], P('rep'), parts along dimension 0
- output 13: float32 [2, 896, 3584], P('rep'), parts along dimension 0
- output 14: float32 [2, 3584, 896], P('rep'), parts along dimension 0
- output 15: float32 [2, 896, 1024], P('rep'), parts along dimension 0
- output 16: float32 [2, 896, 512], P('rep'), parts along dimension 0
- output 17: float32 [2, 896, 512], P('rep'), parts along dimension 0
- output 18: float32 [2, 1024, 896], P('rep'), parts along dimension 0
- output 19: float32 [2, 896, 3584], P('rep'), parts along dimension 0
- output 20: float32 [2, 896, 3584], P('rep'), parts along dimension 0
- output 21: float32 [2, 3584, 896], P('rep'), parts along dimension 0
There are 2 independent parts. The reference program is written for one: setup_inputs(seed, part) draws one part's arguments, and reference() takes and returns one part's arrays. A program takes and returns all parts, laid end to end along the dimension named above; an argument that names none is the same for every part.
All inputs are finite; a program needn't handle non-finite values.
Results may differ from the reference program's by a relative error of at most 0.024.
Values are sent between devices in bfloat16 or wider.
A program may use at most 768 MiB of HBM per device.

```python
import jax
import jax.numpy as jnp
from jax import lax

SEQUENCES = 128
TOKENS = 1024
D = 896
HEADS = 4
KV_HEADS = 2
HEAD = 256
FF = 3584
LAYERS = 1
THETA = 10000
NAMES = ("wq", "wk", "wv", "wo", "w_gate", "w_up", "w_down")
SHAPES = {
    "wq": (LAYERS, D, HEADS * HEAD),
    "wk": (LAYERS, D, KV_HEADS * HEAD),
    "wv": (LAYERS, D, KV_HEADS * HEAD),
    "wo": (LAYERS, HEADS * HEAD, D),
    "w_gate": (LAYERS, D, FF),
    "w_up": (LAYERS, D, FF),
    "w_down": (LAYERS, FF, D),
}


def bump(key, n, height):
    away = (jnp.arange(n, dtype=jnp.int32) - jax.random.randint(key, (), 0, n, jnp.int32)) % n
    return jnp.where(away < n // 8, height, 1.0)


def together(key, own, strength):
    shared = jax.random.normal(key, own.shape[1:], jnp.float32)
    return (own + strength * shared) * lax.rsqrt(1 + strength * strength)


def setup_inputs(seed: int = 0, part: int = 0) -> dict:
    kx, kdy, ka, kb, kz, kf, kh, kl, *keys = jax.random.split(jax.random.key(seed), 8 + 3 * len(NAMES))
    kx, kdy, ka, kb = (jax.random.fold_in(k, part) for k in (kx, kdy, ka, kb))
    kw, km, kv = (keys[i::3] for i in range(3))
    shape = (SEQUENCES, TOKENS, D)
    much_x, much_dy = jax.random.uniform(kz, (2,), jnp.float32, 0.0, 1.0)
    loud = 2.0 ** jax.random.uniform(jax.random.fold_in(kz, 1), (), jnp.float32, -1.0, 2.0)
    layers = 2.0 ** jax.random.uniform(kl, (LAYERS, 1, 1), jnp.float32, -1.0, 1.0)
    times = {"wq": 1.0, "wk": 1.0, "wv": 2.0, "wo": layers, "w_gate": 1.0, "w_up": bump(kh, FF, 4.0), "w_down": layers}
    x = together(ka, jax.random.normal(kx, shape, jnp.float32), much_x) * bump(kf, D, 4.0)
    dy = together(kb, jax.random.normal(kdy, shape, jnp.float32), much_dy)
    drawn = {"x": x.astype(jnp.bfloat16), "dy": (loud * dy * (SEQUENCES * TOKENS) ** -0.5).astype(jnp.bfloat16)}
    for key, name in zip(kw, NAMES, strict=True):
        drawn[name] = (jax.random.normal(key, SHAPES[name], jnp.float32) * SHAPES[name][1] ** -0.5 * times[name]).astype(jnp.bfloat16)
    for key, name in zip(km, NAMES, strict=True):
        drawn[f"m_{name}"] = 0.1 * jax.random.normal(key, SHAPES[name], jnp.float32)
    for key, name in zip(kv, NAMES, strict=True):
        drawn[f"v_{name}"] = jax.random.uniform(key, SHAPES[name], jnp.float32, 0.02, 0.06)
    return drawn


def matmul(a, w):
    return jnp.dot(a, w, preferred_element_type=jnp.float32).astype(jnp.bfloat16)


def normed(h):
    wide = h.astype(jnp.float32)
    scale = lax.rsqrt(jnp.mean(wide**2, -1, keepdims=True) + 1e-6)
    return (wide * scale).astype(jnp.bfloat16)


def turned(t, theta):
    half = t.shape[-1] // 2
    angle = jnp.arange(t.shape[0], dtype=jnp.float32)[:, None] * theta ** (-jnp.arange(half, dtype=jnp.float32) / half)
    cos, sin = jnp.cos(angle)[:, None], jnp.sin(angle)[:, None]
    a, b = t[..., :half].astype(jnp.float32), t[..., half:].astype(jnp.float32)
    return jnp.concatenate([a * cos - b * sin, b * cos + a * sin], -1).astype(jnp.bfloat16)


def seen_by(q, k, v):
    tokens, kv = q.shape[0], k.shape[1]
    q = q.reshape(tokens, kv, -1, q.shape[-1])
    scores = jnp.einsum("tgsd,ugd->gstu", q.astype(jnp.float32), k.astype(jnp.float32)) * q.shape[-1] ** -0.5
    place = jnp.arange(tokens)
    weights = jax.nn.softmax(jnp.where(place[:, None] >= place, scores, -jnp.inf), -1).astype(jnp.bfloat16)
    return jnp.einsum("gstu,ugd->tgsd", weights.astype(jnp.float32), v.astype(jnp.float32)).astype(jnp.bfloat16).reshape(tokens, -1)


def layer(h, w):
    a = normed(h)
    q, k = (turned(matmul(a, w[name]).reshape(h.shape[0], -1, HEAD), THETA) for name in ("wq", "wk"))
    h = h + matmul(seen_by(q, k, matmul(a, w["wv"]).reshape(h.shape[0], -1, HEAD)), w["wo"])
    b = normed(h)
    gate = jnp.dot(b, w["w_gate"], preferred_element_type=jnp.float32)
    up = jnp.dot(b, w["w_up"], preferred_element_type=jnp.float32)
    return h + matmul((jax.nn.silu(gate) * up).astype(jnp.bfloat16), w["w_down"])


def adamw(w, m, v, g):
    m = 0.9 * m + 0.1 * g
    v = 0.95 * v + 0.05 * g * g
    step = m * lax.rsqrt(v + 1e-8) + 0.1 * w
    return (w - 0.02 * step).astype(jnp.bfloat16), m, v


def clipped(gradients, sum_of_squares, count):
    factor = jnp.minimum(1.0, 0.5 * lax.rsqrt(sum_of_squares / count + 1e-30))
    return [g * factor for g in gradients]


def stack(weights, h):
    return lax.scan(lambda h, w: (layer(h, w), None), h, weights)[0]


def reference(x, dy, wq, wk, wv, wo, w_gate, w_up, w_down, m_wq, m_wk, m_wv, m_wo, m_w_gate, m_w_up, m_w_down, v_wq, v_wk, v_wv, v_wo, v_w_gate, v_w_up, v_w_down):
    weights = dict(zip(NAMES, (wq, wk, wv, wo, w_gate, w_up, w_down), strict=True))

    def take(so_far, sequence):
        h, by_y = sequence
        _, back = jax.vjp(stack, weights, h)
        by_weights, by_h = back(by_y)
        return jax.tree.map(lambda total, term: total + term.astype(jnp.float32), so_far, by_weights), by_h

    none_yet = {name: jnp.zeros(w.shape, jnp.float32) for name, w in weights.items()}
    by_weights, by_x = lax.scan(take, none_yet, (x, dy))
    gradients = [by_weights[name].astype(jnp.bfloat16).astype(jnp.float32) for name in NAMES]
    gradients = clipped(gradients, sum(jnp.sum(g * g) for g in gradients), sum(g.size for g in gradients))
    first = (m_wq, m_wk, m_wv, m_wo, m_w_gate, m_w_up, m_w_down)
    second = (v_wq, v_wk, v_wv, v_wo, v_w_gate, v_w_up, v_w_down)
    new = [adamw(weights[name].astype(jnp.float32), m, v, g) for name, m, v, g in zip(NAMES, first, second, gradients, strict=True)]
    return tuple(one[which] for which in range(3) for one in new)
```

```python
import functools
import math

import jax
import jax.numpy as jnp
from jax import lax
from jax.experimental import pallas as pl
from jax.experimental.pallas import tpu as pltpu
from jax.sharding import PartitionSpec as P

THETA = 10000
NAMES = ("wq", "wk", "wv", "wo", "w_gate", "w_up", "w_down")
LANES = 128
STRIPES = 7
NSETS = 6
SUB = 8
TILE = 16
HALF_PART = 64
F32, BF16 = jnp.float32, jnp.bfloat16
VM = 66_000_000
DIMS = {"x": 4, "y": 4, "z": SUB}
ORDER = {"A": ("x", "y", "z"), "B": ("y", "z", "x"), "C": ("z", "x", "y")}
SETS = (("A", -1, 2), ("A", 1, 2), ("B", -1, 2), ("B", 1, 2), ("C", -1, 2), ("C", 1, 1))
WAVE = tuple((c, 0) for c in range(NSETS)) + ((4, 1),) + tuple((c, 1) for c in range(4))


def vm(shape, dtype):
    return pltpu.VMEM(shape, dtype)


def deal(refs, *counts):
    got = []
    for count in counts:
        got.append(refs[:count])
        refs = refs[count:]
    return (*got, refs)


def sizes(cls):
    return tuple(DIMS[d] for d in ORDER[cls])


def devices():
    return math.prod(DIMS.values())


class Place:
    def __init__(self):
        i = lax.axis_index("dp")
        ny, nz = DIMS["y"], DIMS["z"]
        self.at = {"x": i // (ny * nz), "y": (i // nz) % ny, "z": i % nz}
        self.next = {(d, s): self.beside(d, s) for d in DIMS for s in (1, -1)}

    def beside(self, d, s):
        at = {**self.at, d: (self.at[d] + (s + DIMS[d])) % DIMS[d]}
        return {"dp": (at["x"] * DIMS["y"] + at["y"]) * DIMS["z"] + at["z"]}

    def block(self, d, far):
        return (self.at[d] + (far + DIMS[d])) % DIMS[d]

    def slot(self, cls):
        d1, d2, d3 = ORDER[cls]
        return (self.at[d1] * DIMS[d2] + self.at[d2]) * DIMS[d3] + self.at[d3]


def greet(peers):
    barrier = pltpu.get_barrier_semaphore()
    for peer in peers:
        pl.semaphore_signal(barrier, inc=1, device_id=peer)
    pl.semaphore_wait(barrier, len(peers))


def neighbours(me):
    return [me.next[d, s] for d, n in DIMS.items() for s in ((1, -1) if n > 2 else (1,))]


def line_peers(me):
    return [me.beside(d, s) for d, n in DIMS.items() for s in range(1, n)]


def chain(n):
    half = n // 2
    stages = []
    for i in range(1, half + 1):
        far = half - i + 1
        now = [(1, far, None if i == 1 else i - 2, i - 1)]
        if i >= 2:
            now.append((-1, far, None if i == 2 else half + i - 3, half + i - 2))
        stages.append(now)
    return stages, [half - 1] + ([n - 2] if half >= 2 else [])


class Reduce:
    def __init__(self, me, d, sign, own_at, send_at, recv_at, size, sem, step, raw):
        self.me, self.d, self.sign, self.n = me, d, sign, DIMS[d]
        self.own_at, self.send_at, self.recv_at = own_at, send_at, recv_at
        self.size, self.sem, self.step, self.raw = size, sem, min(step, size), raw
        self.stages, self.last = chain(self.n)
        self.first = [0]
        for stage in self.stages:
            self.first.append(self.first[-1] + len(stage))

    def copies(self, stage):
        made = []
        for k, (way, far, _, into) in enumerate(self.stages[stage]):
            s, r = self.sem(self.first[stage] + k)
            made.append(pltpu.make_async_remote_copy(
                self.send_at(self.me.block(self.d, self.sign * way * far), 0, self.size), self.recv_at(into, 0, self.size), s, r,
                device_id=self.me.next[self.d, self.sign * way]))
        return made

    def each(self, body):
        if self.size == self.step:
            body(0)
        else:
            lax.fori_loop(0, self.size // self.step, lambda i, _: body(i * self.step), None)

    def go(self, stage):
        if stage > 0:
            for copy in self.copies(stage - 1):
                copy.wait_recv()
        if stage == len(self.stages):
            return
        for (way, far, joins, _), copy in zip(self.stages[stage], self.copies(stage)):
            block = self.me.block(self.d, self.sign * way * far)
            if joins is not None or not self.raw:
                def body(first):
                    v = self.own_at(block, first, self.step)[...].astype(F32)
                    if joins is not None:
                        v = v + self.recv_at(joins, first, self.step)[...].astype(F32)
                    self.send_at(block, first, self.step)[...] = v.astype(BF16)
                self.each(body)
            copy.start()

    def finish(self, put):
        def body(first):
            v = self.own_at(self.me.at[self.d], first, self.step)[...].astype(F32)
            for r in self.last:
                v = v + self.recv_at(r, first, self.step)[...].astype(F32)
            put(first, self.step, v)
        self.each(body)

    def drain(self):
        for stage in range(len(self.stages)):
            for copy in self.copies(stage):
                copy.wait_send()


class Gather:
    def __init__(self, me, d, sign, block, sem):
        self.me, self.d, self.sign, self.n, self.block, self.sem = me, d, sign, DIMS[d], block, sem
        half = self.n // 2
        self.stages = [[way for way in (1, -1) if stage < half or way == sign] for stage in range(1, half + 1)]
        self.first = [0]
        for stage in self.stages:
            self.first.append(self.first[-1] + len(stage))

    def copies(self, stage):
        made = []
        for k, way in enumerate(self.stages[stage]):
            at = self.block(self.me.block(self.d, -way * stage))
            s, r = self.sem(self.first[stage] + k)
            made.append(pltpu.make_async_remote_copy(at, at, s, r, device_id=self.me.next[self.d, way]))
        return made

    def go(self, stage):
        if stage > 0:
            for copy in self.copies(stage - 1):
                copy.wait_recv()
        if stage < len(self.stages):
            for copy in self.copies(stage):
                copy.start()

    def drain(self):
        for stage in range(len(self.stages)):
            for copy in self.copies(stage):
                copy.wait_send()


class GroupSum:
    def __init__(self, me, ref, sem):
        self.me, self.ref, self.sem = me, ref, sem
        self.steps = len(DIMS) + 1

    def copies(self, n):
        d = list(DIMS)[n]
        before = sum(DIMS[e] - 1 for e in list(DIMS)[:n])
        mine = self.ref.at[n, pl.ds(self.me.at[d], 1)]
        made = []
        for s in range(1, DIMS[d]):
            a, b = self.sem(before + s - 1)
            made.append(pltpu.make_async_remote_copy(mine, mine, a, b, device_id=self.me.beside(d, s)))
        return made

    def go(self, n):
        names = list(DIMS)
        if n > 0:
            for copy in self.copies(n - 1):
                copy.wait_recv()
            total = self.ref[n - 1, 0]
            for i in range(1, DIMS[names[n - 1]]):
                total = total + self.ref[n - 1, i]
            to = self.me.at[names[n]] if n < len(names) else 0
            self.ref[n, pl.ds(to, 1)] = total[None]
            for copy in self.copies(n - 1):
                copy.wait_send()
        if n < len(names):
            for copy in self.copies(n):
                copy.start()


def sends(cls, phase):
    return sizes(cls)[phase] - 1


def bases(phase):
    base = [0]
    for cls, _, _ in SETS:
        base.append(base[-1] + sends(cls, phase))
    return base


class Heavy:
    def __init__(self, me, tb, rx, ssem, rsem, put):
        self.me, self.tb, self.rx, self.ssem, self.rsem, self.put = me, tb, rx, ssem, rsem, put
        self.base = bases(0)

    def ring(self, c, wave, slot):
        cls, sign, k = SETS[c]
        n1, n2, n3 = sizes(cls)
        size = n2 * n3
        at = lambda block, first, step: self.tb[c].at[slot, pl.ds(block * size + first, step)]
        return Reduce(self.me, ORDER[cls][0], sign, at, at, lambda i, first, step: self.rx[c].at[wave, i, pl.ds(first, step)], size,
                      lambda j: (self.ssem.at[wave, self.base[c] + j], self.rsem.at[wave, self.base[c] + j]), SUB, True)

    def step(self, wave, slot, quarter):
        for c, (cls, _, _) in enumerate(SETS):
            stages = sizes(cls)[0] // 2
            pace = 4 // stages
            if quarter % pace == 0:
                ring = self.ring(c, wave, slot)
                ring.go(quarter // pace)
                if quarter == 4:
                    ring.finish(functools.partial(self.put, c, wave))
                    ring.drain()


def heavy_buffers(slots, waves):
    tb, rx = [], []
    for cls, _, k in SETS:
        n1, n2, n3 = sizes(cls)
        tb.append(vm((slots, devices(), k, SUB, LANES), BF16))
        rx.append(vm((waves, n1 - 1, n2 * n3, k, SUB, LANES), BF16))
    return tb + rx


def heavy_sems(waves):
    return [pltpu.SemaphoreType.DMA((waves, bases(0)[-1]))] * 2


def sum_shapes(waves):
    return [(waves, sizes(cls)[1] * sizes(cls)[2], k, SUB, LANES) for cls, _, k in SETS]


def heavy_loop(waves, heavy, slots, compute):
    lag = (0, 2, 4, NSETS, SUB)

    def at_point(i, p):
        for q in reversed(range(len(lag))):
            if (p - 2 - lag[q]) % 3 == 0:
                w = i + (p - 2 - lag[q]) // 3

                @pl.when((w >= 0) & (w < waves))
                def _():
                    heavy.step(w, w % slots, q)

    def body(i, _):
        @pl.when(i < waves)
        def _():
            compute(i, functools.partial(at_point, i))

        @pl.when(i >= waves)
        def _():
            for p in range(3):
                at_point(i, p)

    lax.fori_loop(0, waves + 3, body, None)


TICKS = 1 + max((sizes(cls)[1] + sizes(cls)[2]) // 2 for cls, _, _ in SETS)
FF_CHUNK = 512
TOKEN_BLOCK = 512


def ffn_kernel(waves, x_ref, dy_ref, wg_ref, wu_ref, wd_ref, *refs):
    sums, (db_ref, *refs) = deal(refs, NSETS)
    tb, rx, acc, rest = deal(refs, NSETS, NSETS, NSETS)
    ssem, rsem, wbuf, wdbuf, hid_s, dg_s, du_s, dbg, dbu, wsem, osem = rest
    me = Place()
    slots = tb[0].shape[0]

    def weights(j, s):
        cols = pl.ds(pl.multiple_of(j * FF_CHUNK, FF_CHUNK), FF_CHUNK)
        return [pltpu.make_async_copy(wg_ref.at[0, :, cols], wbuf.at[s, 0], wsem.at[s, 0]),
                pltpu.make_async_copy(wu_ref.at[0, :, cols], wbuf.at[s, 1], wsem.at[s, 1]),
                pltpu.make_async_copy(wd_ref.at[0, cols, :], wdbuf.at[s], wsem.at[s, 2])]

    for copy in weights(0, 0):
        copy.start()
    dbg[...] = jnp.zeros_like(dbg)
    dbu[...] = jnp.zeros_like(dbu)
    pad_c, pad_k = WAVE[10]
    for s in range(slots):
        tb[pad_c][s, devices() // 2:, pad_k] = jnp.zeros((devices() // 2, SUB, LANES), BF16)
    greet(neighbours(me))

    def keep(c, wave):
        return pltpu.make_async_copy(acc[c].at[wave % 2], sums[c].at[wave], osem.at[wave % 2, c])

    def put(c, wave, first, step, v):
        if isinstance(first, int) and first == 0 and step == sums[c].shape[1]:
            acc[c][wave % 2] = v
        else:
            acc[c][wave % 2, pl.ds(first, step)] = v

    heavy = Heavy(me, tb, rx, ssem, rsem, put)

    def compute(j, now):
        s = j % 2
        slot = j % slots
        for copy in weights(j, s):
            copy.wait()

        @pl.when(j + 1 < waves)
        def _():
            for copy in weights(j + 1, 1 - s):
                copy.start()

        def tokens(n, _):
            rows = pl.ds(pl.multiple_of(n * TOKEN_BLOCK, TOKEN_BLOCK), TOKEN_BLOCK)
            b = x_ref[rows, :]
            gate = _dot(b, wbuf[s, 0], 1, 0)
            up = _dot(b, wbuf[s, 1], 1, 0)
            dh = _dot(dy_ref[rows, :], wdbuf[s], 1, 1).astype(BF16).astype(F32)
            sig = 1.0 / (1.0 + jnp.exp(-gate))
            silu = gate * sig
            hid_s[rows, :] = (silu * up).astype(BF16)
            du_s[rows, :] = (dh * silu).astype(BF16)
            dg_s[rows, :] = (dh * up * (sig + silu * (1.0 - sig))).astype(BF16)

        now(0)
        lax.fori_loop(0, x_ref.shape[0] // TOKEN_BLOCK, tokens, None)
        now(1)
        for half, src in enumerate((dg_s, du_s)):
            g = _dot(x_ref[...], src[...], 0, 0).astype(BF16)
            for t in range(STRIPES):
                c, k = WAVE[t]
                for i in range(4):
                    tb[c][slot, pl.ds(HALF_PART * half + TILE * i, TILE), k] = g[LANES * t : LANES * t + LANES, LANES * i : LANES * i + LANES].reshape(TILE, SUB, LANES)
        g = _dot(hid_s[...], dy_ref[...], 0, 0).astype(BF16)
        for i in range(STRIPES):
            c, k = WAVE[STRIPES + i // 2]
            tb[c][slot, pl.ds(HALF_PART * (i % 2), HALF_PART), k] = g[:, LANES * i : LANES * i + LANES].reshape(HALF_PART, SUB, LANES)
        now(2)
        dbg[...] += _dot(dg_s[...], wbuf[s, 0], 1, 1)
        dbu[...] += _dot(du_s[...], wbuf[s, 1], 1, 1)

    class Kept(Heavy):
        def step(self, wave, slot, quarter):
            if quarter == 4:
                @pl.when(wave >= 2)
                def _():
                    for c in range(NSETS):
                        keep(c, wave - 2).wait()
            super().step(wave, slot, quarter)
            if quarter == 4:
                for c in range(NSETS):
                    keep(c, wave).start()

    heavy_loop(waves, Kept(me, tb, rx, ssem, rsem, put), slots, compute)
    for wave in (waves - 2, waves - 1):
        for c in range(NSETS):
            keep(c, wave).wait()
    db_ref[...] = (dbg[...].astype(BF16).astype(F32) + dbu[...].astype(BF16).astype(F32)).astype(BF16)


def ffn_call(b, dy, wg, wu, wd):
    waves = wg.shape[2] // FF_CHUNK
    tokens, d = b.shape
    whole = pl.BlockSpec(memory_space=pltpu.VMEM)
    anywhere = pl.BlockSpec(memory_space=pl.ANY)
    mid = vm((tokens, FF_CHUNK), BF16)
    return pl.pallas_call(
        functools.partial(ffn_kernel, waves),
        out_shape=[jax.ShapeDtypeStruct(s, F32) for s in sum_shapes(waves)] + [jax.ShapeDtypeStruct((tokens, d), BF16)],
        in_specs=[whole, whole, anywhere, anywhere, anywhere],
        out_specs=[anywhere] * NSETS + [whole],
        scratch_shapes=heavy_buffers(4, waves) + [vm((2, *s[1:]), F32) for s in sum_shapes(waves)] + heavy_sems(waves) + [
            vm((2, 2, d, FF_CHUNK), BF16), vm((2, FF_CHUNK, d), BF16), mid, mid, mid, vm((tokens, d), F32), vm((tokens, d), F32),
            pltpu.SemaphoreType.DMA((2, 3)), pltpu.SemaphoreType.DMA((2, NSETS))],
        compiler_params=pltpu.CompilerParams(collective_id=0, has_side_effects=True, vmem_limit_bytes=VM),
        cost_estimate=pl.CostEstimate(flops=TILE * tokens * d * wg.shape[2], transcendentals=tokens * wg.shape[2], bytes_accessed=40_000_000),
    )(b, dy, wg, wu, wd)


def gather_kernel(ffn_waves, own_waves, *refs):
    waves = ffn_waves + own_waves
    acc_in, tb_in, g_out, (tot_out, *refs) = deal(refs, NSETS, NSETS, NSETS)
    g, tb, rx, rx2, rx3, rest = deal(refs, NSETS, NSETS, NSETS, NSETS, NSETS)
    ssem, rsem, nrm, lsem, osem, l2s, l2r, l3s, l3r, g3s, g3r, g2s, g2r, g1s, g1r, ns, nr = rest
    me = Place()

    def first_part(acc2, send2, acc3, send3):
        for c in range(NSETS):
            pltpu.make_async_copy(tb_in[c], tb[c], lsem.at[c, 0]).start()
            pltpu.make_async_copy(acc_in[c], acc2[c].at[pl.ds(0, ffn_waves)], lsem.at[c, 1]).start()
        greet(line_peers(me))
        for c in range(NSETS):
            pltpu.make_async_copy(tb_in[c], tb[c], lsem.at[c, 0]).wait()
            pltpu.make_async_copy(acc_in[c], acc2[c].at[pl.ds(0, ffn_waves)], lsem.at[c, 1]).wait()

        def put(c, wave, first, step, v):
            acc2[c][ffn_waves + wave, pl.ds(first, step)] = v

        heavy = Heavy(me, tb, rx, ssem, rsem, put)
        rings = {}
        for part, (w0, dw) in enumerate(((0, ffn_waves), (ffn_waves, own_waves))):
            wr = pl.ds(w0, dw)
            for c, (cls, sign, k) in enumerate(SETS):
                d1, d2, d3 = ORDER[cls]
                n1, n2, n3 = sizes(cls)
                b2, b3 = bases(1), bases(2)
                rings[part, c] = (
                    Reduce(me, d2, sign,
                           lambda b, f, st, c=c, wr=wr, n3=n3: acc2[c].at[wr, pl.ds(b * n3 + f, st)],
                           lambda b, f, st, c=c, wr=wr, n3=n3: send2[c].at[wr, pl.ds(b * n3 + f, st)],
                           lambda i, f, st, c=c, wr=wr: rx2[c].at[i, wr, pl.ds(f, st)],
                           n3, lambda j, c=c, part=part, b2=b2: (l2s.at[part, b2[c] + j], l2r.at[part, b2[c] + j]), 1, False),
                    Reduce(me, d3, sign,
                           lambda b, f, st, c=c, wr=wr: acc3[c].at[wr, pl.ds(b + f, st)],
                           lambda b, f, st, c=c, wr=wr: send3[c].at[wr, pl.ds(b + f, st)],
                           lambda i, f, st, c=c, wr=wr: rx3[c].at[i, wr, pl.ds(f, st)],
                           1, lambda j, c=c, part=part, b3=b3: (l3s.at[part, b3[c] + j], l3r.at[part, b3[c] + j]), 1, False))

        def light(part, tick):
            wr = pl.ds(*((0, ffn_waves) if part == 0 else (ffn_waves, own_waves)))
            for c, (cls, sign, k) in enumerate(SETS):
                n1, n2, n3 = sizes(cls)
                h2, h3 = n2 // 2, n3 // 2
                two, three = rings[part, c]
                if tick <= h2:
                    two.go(tick)
                    if tick == h2:
                        def put3(first, step, v, c=c, wr=wr):
                            acc3[c][wr, pl.ds(first, step)] = v
                        two.finish(put3)
                        three.go(0)
                elif tick <= h2 + h3:
                    three.go(tick - h2)
                    if tick == h2 + h3:
                        slot = me.slot(cls)
                        def putg(first, step, v, c=c, wr=wr, slot=slot):
                            g[c][wr, pl.ds(slot, 1)] = v.astype(BF16)
                        three.finish(putg)
                        two.drain()
                        three.drain()

        for tick in range(TICKS):
            light(0, tick)
            if tick < 5:
                for w in range(own_waves):
                    heavy.step(w, w, tick)
            else:
                light(1, tick - 5)
        second = TICKS - 5
        for tick in range(TICKS):
            spread(0, tick)
            if second < TICKS:
                light(1, second)
                second += 1

    def spread(part, tick):
        for c, (cls, sign, k) in enumerate(SETS):
            d1, d2, d3 = ORDER[cls]
            n1, n2, n3 = sizes(cls)
            wr = pl.ds(*((0, ffn_waves) if part == 0 else (ffn_waves, own_waves)))
            b2, b3 = bases(1)[c], bases(2)[c]
            at3 = (me.at[d1] * n2 + me.at[d2]) * n3
            at2 = me.at[d1] * n2
            three = Gather(me, d3, sign, lambda i: g[c].at[wr, pl.ds(at3 + i, 1)], lambda j: (g3s.at[part, b3 + j], g3r.at[part, b3 + j]))
            two = Gather(me, d2, sign, lambda i: g[c].at[wr, pl.ds((at2 + i) * n3, n3)], lambda j: (g2s.at[part, b2 + j], g2r.at[part, b2 + j]))
            h3, h2 = n3 // 2, n2 // 2
            if tick <= h3:
                three.go(tick)
            if h3 <= tick <= h3 + h2:
                two.go(tick - h3)
                if tick == h3 + h2:
                    three.drain()
                    two.drain()

    shapes2 = sum_shapes(waves)
    shapes3 = [(waves, sizes(cls)[2], k, SUB, LANES) for cls, _, k in SETS]
    pl.run_scoped(lambda *b: first_part(*deal(b, NSETS, NSETS, NSETS)),
                  *[vm(s, F32) for s in shapes2], *[vm(s, BF16) for s in shapes2], *[vm(s, F32) for s in shapes3], *[vm(s, BF16) for s in shapes3])

    total = jnp.zeros((SUB, LANES), F32)
    for c, (cls, _, k) in enumerate(SETS):
        v = g[c][:, me.slot(cls)].astype(F32)
        total = total + jnp.sum(v * v, axis=(0, 1))
    nrm[0, pl.ds(me.at["x"], 1)] = total[None]
    summing = GroupSum(me, nrm, lambda j: (ns.at[j], nr.at[j]))
    def heavy_gather(c, wave):
        cls, sign, k = SETS[c]
        n1, n2, n3 = sizes(cls)
        size = n2 * n3
        b1 = bases(0)
        return Gather(me, ORDER[cls][0], sign, lambda i: g[c].at[wave, pl.ds(i * size, size)],
                      lambda j: (g1s.at[wave, b1[c] + j], g1r.at[wave, b1[c] + j]))

    def quarter_of(wave, quarter):
        for c, (cls, _, _) in enumerate(SETS):
            pace = 4 // (sizes(cls)[0] // 2)
            if quarter % pace == 0:
                ring = heavy_gather(c, wave)
                ring.go(quarter // pace)
                if quarter == 4:
                    ring.drain()
                    pltpu.make_async_copy(g[c].at[wave], g_out[c].at[wave], osem.at[c, wave]).start()

    def guarded(i, lag, quarter):
        w = i - lag

        @pl.when((w >= 0) & (w < waves))
        def _():
            quarter_of(w, quarter)

    def body(i, _):
        for quarter in reversed(range(5)):
            guarded(i, quarter, quarter)
        for tick in range(TICKS):
            @pl.when(i == tick)
            def _():
                spread(1, tick)
                if tick < summing.steps:
                    summing.go(tick)

    lax.fori_loop(0, waves + 4, body, None)
    tot_out[...] = nrm[len(DIMS), 0]

    def done(w, _):
        for c in range(NSETS):
            pltpu.make_async_copy(g[c].at[w], g_out[c].at[w], osem.at[c, w]).wait()
    lax.fori_loop(0, waves, done, None)


def gather_call(sums, own, ffn_waves, own_waves):
    waves = ffn_waves + own_waves
    gs = [(waves, devices(), k, SUB, LANES) for _, _, k in SETS]
    s2, s3 = [], []
    for cls, _, k in SETS:
        n1, n2, n3 = sizes(cls)
        s2.append((n2 - 1, waves, n3, k, SUB, LANES))
        s3.append((n3 - 1, waves, 1, k, SUB, LANES))
    dma = pltpu.SemaphoreType.DMA
    n1, n2, n3 = (bases(p)[-1] for p in range(3))
    peers = sum(n - 1 for n in DIMS.values())
    anywhere = pl.BlockSpec(memory_space=pl.ANY)
    return pl.pallas_call(
        functools.partial(gather_kernel, ffn_waves, own_waves),
        out_shape=[jax.ShapeDtypeStruct(s, BF16) for s in gs] + [jax.ShapeDtypeStruct((SUB, LANES), F32)],
        in_specs=[anywhere] * 12,
        out_specs=[anywhere] * NSETS + [pl.BlockSpec(memory_space=pltpu.VMEM)],
        scratch_shapes=[vm(s, BF16) for s in gs] + heavy_buffers(own_waves, own_waves) + [vm(s, BF16) for s in s2 + s3] + heavy_sems(own_waves) + [
            vm((4, SUB, SUB, LANES), F32), dma((NSETS, 2)), dma((NSETS, waves))] + [dma(s) for s in ((2, n2), (2, n3), (2, n3), (2, n2), (waves, n1), (peers,)) for _ in "sr"],
        compiler_params=pltpu.CompilerParams(collective_id=1, has_side_effects=True, vmem_limit_bytes=VM),
        cost_estimate=pl.CostEstimate(flops=10_000_000_000, transcendentals=0, bytes_accessed=60_000_000),
    )(*sums, *own)


COUNT = 12386304
FFN_WAVES, OWN_WAVES = STRIPES, 2


def attention_parts():
    return [(kind, t) for kind in ("o", "kv", "q") for t in range(STRIPES)]


def place_of(kind, j, t):
    if kind in ("gu", "d"):
        c, k = WAVE[t if kind == "gu" else STRIPES + t]
        return c, j, k
    n = attention_parts().index((kind, t))
    c, k = WAVE[n % 11]
    return c, FFN_WAVES + n // 11, k


def adam_jobs():
    jobs = []
    for kind, j in [("gu" if h == 0 else "d", j) for j in range(FFN_WAVES) for h in (0, 1)] + [("o", 0), ("q", 0), ("kv", 0)]:
        if kind in ("gu", "q", "kv"):
            for t in range(STRIPES):
                rows = LANES * t
                pieces = {"gu": [(4, rows, 512 * j, 512, 0), (5, rows, 512 * j, 512, 512)], "q": [(0, rows, 0, 1024, 0)],
                          "kv": [(1, rows, 0, 512, 0), (2, rows, 0, 512, 512)]}[kind]
                jobs.append((pieces, [(*place_of(kind, j, t), TILE * i) for i in range(SUB)]))
        elif kind == "o":
            for b in range(SUB):
                jobs.append(([(3, LANES * b, 0, 896, 0)], [(*place_of(kind, j, t), TILE * b) for t in range(STRIPES)]))
        else:
            for b in range(4):
                jobs.append(([(NSETS, 512 * j + LANES * b, 0, 896, 0)], [(*place_of(kind, j, t // 2), HALF_PART * (t % 2) + TILE * b) for t in range(STRIPES)]))
    return jobs


def adam_kernel(depth, *refs):
    n = len(NAMES)
    w, m, v, (tot, *refs) = deal(refs, n, n, n)
    g_in, wo, mo, vo, g, rest = deal(refs, NSETS, n, n, n, NSETS)
    wb, mb, vb, wn, mn, vn, isem, osem, gsem = rest
    jobs = adam_jobs()
    waves = FFN_WAVES + OWN_WAVES

    def load(wave):
        return [pltpu.make_async_copy(g_in[c].at[wave], g[c].at[wave], gsem.at[c, wave]) for c in range(NSETS)]

    def moves(i, sides, bufs, sem, out):
        s = i % depth
        made = []
        for n, (which, row, col, width, at) in enumerate(jobs[i][0]):
            for a, (side, buf) in enumerate(zip(sides, bufs)):
                far, near = side[which].at[0, pl.ds(row, LANES), pl.ds(col, width)], buf.at[s, :, pl.ds(at, width)]
                made.append(pltpu.make_async_copy(near, far, sem.at[s, n, a]) if out else pltpu.make_async_copy(far, near, sem.at[s, n, a]))
        return made

    ins = lambda i: moves(i, (w, m, v), (wb, mb, vb), isem, False)
    outs = lambda i: moves(i, (wo, mo, vo), (wn, mn, vn), osem, True)

    for copy in load(0):
        copy.start()
    for i in range(depth - 1):
        for copy in ins(i):
            copy.start()
    for copy in load(1):
        copy.start()
    square = jnp.sum(tot[...], keepdims=True)
    factor = jnp.broadcast_to(jnp.minimum(1.0, 0.5 * lax.rsqrt(square / COUNT + 1e-30)), (TILE, LANES))
    have = 0
    for i, (pieces, tiles) in enumerate(jobs):
        s = i % depth
        while have <= max(t[1] for t in tiles):
            for copy in load(have):
                copy.wait()
            if have + 2 < waves:
                for copy in load(have + 2):
                    copy.start()
            have += 1
        if i + depth - 1 < len(jobs):
            for copy in ins(i + depth - 1):
                copy.start()
        for copy in ins(i):
            copy.wait()
        if i >= depth:
            for copy in outs(i - depth):
                copy.wait()

        def body(r, _):
            rows = pl.ds(pl.multiple_of(TILE * r, TILE), TILE)
            for n, (c, wave, k, slot) in enumerate(tiles):
                cols = slice(LANES * n, LANES * n + LANES)
                x = g[c][wave, pl.ds(slot + 2 * r, 2), k].astype(F32).reshape(TILE, LANES) * factor
                a = 0.9 * mb[s, rows, cols] + 0.1 * x
                b = 0.95 * vb[s, rows, cols] + 0.05 * x * x
                old = wb[s, rows, cols].astype(F32)
                mn[s, rows, cols] = a
                vn[s, rows, cols] = b
                wn[s, rows, cols] = (old - 0.02 * (a * lax.rsqrt(b + 1e-8) + 0.1 * old)).astype(BF16)

        lax.fori_loop(0, SUB, body, None)
        for copy in outs(i):
            copy.start()
    for i in range(len(jobs) - depth, len(jobs)):
        for copy in outs(i):
            copy.wait()


def adam_call(w, m, v, tot, gs, depth=4):
    anywhere = pl.BlockSpec(memory_space=pl.ANY)
    buf = lambda t: vm((depth, LANES, 1024), t)
    dma = pltpu.SemaphoreType.DMA
    return pl.pallas_call(
        functools.partial(adam_kernel, depth),
        out_shape=[jax.ShapeDtypeStruct(x.shape, x.dtype) for x in (*w, *m, *v)],
        in_specs=[anywhere] * 21 + [pl.BlockSpec(memory_space=pltpu.VMEM)] + [anywhere] * NSETS,
        out_specs=[anywhere] * 21,
        scratch_shapes=[vm(x.shape, BF16) for x in gs] + [buf(BF16), buf(F32), buf(F32)] * 2
        + [dma((depth, 2, 3)), dma((depth, 2, 3)), dma((NSETS, FFN_WAVES + OWN_WAVES))],
        compiler_params=pltpu.CompilerParams(vmem_limit_bytes=VM),
        cost_estimate=pl.CostEstimate(flops=25 * COUNT, transcendentals=COUNT, bytes_accessed=270_000_000),
    )(*w, *m, *v, tot, *gs)


HEAD, GROUPS, PER = 256, 2, 2
QB = 256
LOG2E = 1.4426950408889634


def _dot(a, b, ca, cb):
    return lax.dot_general(a, b, (((ca,), (cb,)), ((), ())), preferred_element_type=F32)


def root(wide):
    return lax.rsqrt(jnp.mean(wide * wide, -1, keepdims=True) + 1e-6)


def turn(t, cos, sin):
    a, b = t[:, : HEAD // 2], t[:, HEAD // 2 :]
    return jnp.concatenate([a * cos - b * sin, b * cos + a * sin], -1)


def stacked(ref, rows, g):
    return jnp.concatenate([ref[rows, HEAD * h : HEAD * h + HEAD] for h in range(PER * g, PER * g + PER)], 0)


def hidden(s, fill):
    n = s.shape[0]
    own = s[n - QB :]
    key = lax.broadcasted_iota(jnp.int32, own.shape, 0)
    query = lax.broadcasted_iota(jnp.int32, own.shape, 1) % QB
    own = jnp.where(key <= query, own, fill)
    return own if n == QB else jnp.concatenate([s[: n - QB], own], 0)


def forward_kernel(x, wq, wk, wv, wo, cos, sin, a_o, q_o, k_o, v_o, out_o, lse_o, h_o, b_o):
    tokens = x.shape[0]
    big = 512

    def project(n, _):
        rows = pl.ds(pl.multiple_of(n * big, big), big)
        wide = x[rows, :].astype(F32)
        a = (wide * root(wide)).astype(BF16)
        a_o[rows, :] = a
        c, s = cos[rows, :], sin[rows, :]
        for w, to in ((wq, q_o), (wk, k_o)):
            t = _dot(a, w[0], 1, 0).astype(BF16).astype(F32)
            for at in range(0, t.shape[1], HEAD):
                to[rows, at : at + HEAD] = turn(t[:, at : at + HEAD], c, s).astype(BF16)
        v_o[rows, :] = _dot(a, wv[0], 1, 0).astype(BF16)

    lax.fori_loop(0, tokens // big, project, None)
    e = HEAD**-0.5 * LOG2E
    for g in range(GROUPS):
        cols = slice(HEAD * g, HEAD * g + HEAD)
        for i in range(tokens // QB):
            rows, n = slice(QB * i, QB * i + QB), QB * (i + 1)
            s = hidden(_dot(k_o[:n, cols], stacked(q_o, rows, g), 1, 1), -1e30)
            top = s.max(0, keepdims=True)
            p = jnp.exp2((s - top) * e)
            total = p.sum(0, keepdims=True)
            p = (p * (1.0 / total)).astype(BF16)
            out = _dot(v_o[:n, cols], p, 0, 0).T.astype(BF16)
            lse = top * e + jnp.log2(total)
            for h in range(PER):
                out_o[rows, HEAD * (PER * g + h) : HEAD * (PER * g + h + 1)] = out[QB * h : QB * h + QB]
                lse_o[PER * g + h : PER * g + h + 1, rows] = lse[:, QB * h : QB * h + QB]

    def finish(n, _):
        rows = pl.ds(pl.multiple_of(n * big, big), big)
        h = (x[rows, :].astype(F32) + _dot(out_o[rows, :], wo[0], 1, 0).astype(BF16).astype(F32)).astype(BF16)
        h_o[rows, :] = h
        wide = h.astype(F32)
        b_o[rows, :] = (wide * root(wide)).astype(BF16)

    lax.fori_loop(0, tokens // big, finish, None)


def forward_call(x, wq, wk, wv, wo, cos, sin):
    tokens, d = x.shape
    out = lambda n: jax.ShapeDtypeStruct((tokens, n), BF16)
    nq, nk = wq.shape[2], wk.shape[2]
    whole = pl.BlockSpec(memory_space=pltpu.VMEM)
    return pl.pallas_call(
        forward_kernel,
        out_shape=[out(d), out(nq), out(nk), out(nk), out(nq), jax.ShapeDtypeStruct((nq // HEAD, tokens), F32), out(d), out(d)],
        in_specs=[whole] * STRIPES,
        out_specs=[whole] * SUB,
        compiler_params=pltpu.CompilerParams(vmem_limit_bytes=VM),
        cost_estimate=pl.CostEstimate(flops=12_000_000_000, transcendentals=4_000_000, bytes_accessed=25_000_000),
    )(x, wq, wk, wv, wo, cos, sin)


def own_place(kind, t):
    c, wave, k = place_of(kind, 0, t)
    return c, wave - FFN_WAVES, k


def backward_pieces(refs):
    r = refs
    tokens = r.dy.shape[0]
    big = 512
    e, scale = HEAD**-0.5 * LOG2E, HEAD**-0.5

    def by_norm(n):
        def run():
            rows = slice(n * big, n * big + big)
            wide = r.h[rows, :].astype(F32)
            by = r.by_b[rows, :].astype(F32)
            s = root(wide)
            back = by * s - wide * (s * s * s * jnp.mean(by * wide, -1, keepdims=True))
            r.by_h[rows, :] = (r.dy[rows, :].astype(F32) + back.astype(BF16).astype(F32)).astype(BF16)
            r.by_out[rows, :] = _dot(r.by_h[rows, :], r.wo[0], 1, 1).astype(BF16)
        return run

    def by_wo():
        g = _dot(r.out[...], r.by_h[...], 0, 0).astype(BF16)
        for t in range(STRIPES):
            c, w, k = own_place("o", t)
            r.own[c][w, :, k] = g[:, LANES * t : LANES * t + LANES].reshape(devices(), SUB, LANES)

    def attend(g, i):
        cols = slice(HEAD * g, HEAD * g + HEAD)
        rows, n = slice(QB * i, QB * i + QB), QB * (i + 1)

        def run():
            q, do = stacked(r.q, rows, g), stacked(r.by_out, rows, g)
            lse = jnp.concatenate([r.lse[h : h + 1, rows] for h in range(PER * g, PER * g + PER)], 1)
            p = hidden(jnp.exp2(_dot(r.k[:n, cols], q, 1, 1) * e - lse), 0.0)
            dp = _dot(r.v[:n, cols], do, 1, 1)
            delta = (p * dp).sum(0, keepdims=True)
            ds = (p * (dp - delta)).astype(BF16)
            r.by_v[:n, cols] += _dot(p.astype(BF16), do, 1, 0)
            r.by_k[:n, cols] += _dot(ds, q, 1, 0)
            dq = (_dot(r.k[:n, cols], ds, 0, 0) * scale).T.astype(BF16).astype(F32)
            for h in range(PER):
                at = HEAD * (PER * g + h)
                r.by_q[rows, at : at + HEAD] = turn(dq[QB * h : QB * h + QB], r.cos[rows, :], -r.sin[rows, :]).astype(BF16)
        return run

    def clear():
        r.by_k[...] = jnp.zeros_like(r.by_k)
        r.by_v[...] = jnp.zeros_like(r.by_v)

    def by_w(kind, cols, first, make):
        def run():
            g = _dot(r.a[...], make(cols), 0, 0).astype(BF16)
            for t in range(STRIPES):
                c, w, k = own_place(kind, t)
                for n in range(g.shape[1] // LANES):
                    r.own[c][w, pl.ds(TILE * (first + n), TILE), k] = g[LANES * t : LANES * t + LANES, LANES * n : LANES * n + LANES].reshape(TILE, SUB, LANES)
        return run

    def keys(cols):
        return jnp.concatenate([turn((r.by_k[:, at : at + HEAD] * scale).astype(BF16).astype(F32), r.cos[...], -r.sin[...]).astype(BF16)
                                for at in range(cols.start, cols.stop, HEAD)], 1)

    pieces = [clear, *(by_norm(n) for n in range(tokens // big)), by_wo]
    pieces += [attend(g, i) for g in range(GROUPS) for i in range(tokens // QB)]
    half = slice(0, GROUPS * HEAD)
    pieces += [by_w("kv", half, 4, lambda cols: r.by_v[:, cols].astype(BF16)), by_w("kv", half, 0, keys)]
    pieces += [by_w("q", slice(at, at + 512), at // LANES, lambda cols: r.by_q[:, cols]) for at in range(0, GROUPS * PER * HEAD, 512)]
    return pieces


class Names:
    def __init__(self, **refs):
        self.__dict__.update(refs)


BACKWARD = ("dy", "h", "by_b", "a", "q", "k", "v", "out", "lse", "wo", "cos", "sin")
BACKWARD_SCRATCH = ("by_h", "by_out", "by_q", "by_k", "by_v")


def backward_scratch(tokens, d):
    wide, key = GROUPS * PER * HEAD, GROUPS * HEAD
    return [vm((tokens, d), BF16), vm((tokens, wide), BF16), vm((tokens, wide), BF16), vm((tokens, key), F32), vm((tokens, key), F32)]


def backward_kernel(*refs):
    n = len(BACKWARD)
    names = dict(zip(BACKWARD, refs[:n]))
    own = refs[n : n + NSETS]
    names.update(zip(BACKWARD_SCRATCH, refs[n + NSETS :]))
    pad = WAVE[10]
    own[pad[0]][OWN_WAVES - 1, :, pad[1]] = jnp.zeros((devices(), SUB, LANES), BF16)
    for piece in backward_pieces(Names(own=own, **names)):
        piece()


def backward_call(*given):
    tokens, d = given[0].shape
    whole = pl.BlockSpec(memory_space=pltpu.VMEM)
    return pl.pallas_call(
        backward_kernel,
        out_shape=[jax.ShapeDtypeStruct((OWN_WAVES, devices(), k, SUB, LANES), BF16) for _, _, k in SETS],
        in_specs=[whole] * len(given),
        out_specs=[whole] * NSETS,
        scratch_shapes=backward_scratch(tokens, d),
        compiler_params=pltpu.CompilerParams(vmem_limit_bytes=VM),
        cost_estimate=pl.CostEstimate(flops=18_000_000_000, transcendentals=4_000_000, bytes_accessed=25_000_000),
    )(*given)


def rotation(tokens):
    half = HEAD // 2
    angle = jnp.arange(tokens, dtype=F32)[:, None] * THETA ** (-jnp.arange(half, dtype=F32) / half)
    return jnp.cos(angle), jnp.sin(angle)


def solution(mesh):
    def step(x, dy, *arrays):
        n = len(NAMES)
        w, m, v = (arrays[n * i : n * i + n] for i in range(3))
        wq, wk, wv, wo, gate, up, down = w
        x, dy = x[0], dy[0]
        turns = rotation(x.shape[0])
        a, q, k, value, out, lse, h, b = forward_call(x, wq, wk, wv, wo, *turns)
        *sums, by_b = ffn_call(b, dy, gate, up, down)
        own = backward_call(dy, h, by_b, a, q, k, value, out, lse, wo, *turns)
        *gs, total = gather_call(sums, own, FFN_WAVES, OWN_WAVES)
        return tuple(adam_call(w, m, v, total, gs))

    states, all_of = P(("rep", "dp"), None, None), P(None, None, None)
    return jax.shard_map(
        step,
        mesh=mesh,
        in_specs=(states, states) + (all_of,) * 21,
        out_specs=(P("rep", None, None),) * 21,
        check_vma=False,
    )
```

```python
import functools
import math

import jax
import jax.numpy as jnp
from jax import lax
from jax.experimental import pallas as pl
from jax.experimental.pallas import tpu as pltpu
from jax.sharding import PartitionSpec as P

THETA = 10000
NAMES = ("wq", "wk", "wv", "wo", "w_gate", "w_up", "w_down")
PAIR = 2
LANES = 128
STRIPES = 7
NSETS = 6
SUB = 8
TILE = 16
HALF_PART = 64
F32, BF16 = jnp.float32, jnp.bfloat16
VM = 66_000_000


def room(*arrays):
    return VM - sum(math.prod(a.shape) * jnp.dtype(a.dtype).itemsize for a in arrays)
DIMS = {"x": 4, "y": 4, "z": SUB}
ORDER = {"A": ("x", "y", "z"), "B": ("y", "x", "z"), "C": ("z", "x", "y")}
SETS = (("A", -1, PAIR), ("A", 1, PAIR), ("B", -1, PAIR), ("B", 1, PAIR), ("C", -1, PAIR), ("C", 1, 1))
WAVE = tuple((c, 0) for c in range(NSETS)) + ((4, 1),) + tuple((c, 1) for c in range(4))


def vm(shape, dtype):
    return pltpu.VMEM(shape, dtype)


def in_vmem(arrays):
    return [pltpu.with_memory_space_constraint(a, pltpu.VMEM) for a in arrays]


def deal(refs, *counts):
    got = []
    for count in counts:
        got.append(refs[:count])
        refs = refs[count:]
    return (*got, refs)


def sizes(cls):
    return tuple(DIMS[d] for d in ORDER[cls])


def devices():
    return math.prod(DIMS.values())


class Place:
    def __init__(self):
        i = lax.axis_index("dp")
        ny, nz = DIMS["y"], DIMS["z"]
        self.at = {"x": i // (ny * nz), "y": (i // nz) % ny, "z": i % nz}
        self.places = {(d, far): (self.at[d] + far) % n if far else self.at[d] for d, n in DIMS.items() for far in range(n)}
        self.peers = {}
        for d, far in self.places:
            at = {**self.at, d: self.places[d, far]}
            self.peers[d, far] = {"dp": (at["x"] * ny + at["y"]) * nz + at["z"]}

    def beside(self, d, far):
        return self.peers[d, far % DIMS[d]]

    def block(self, d, far):
        return self.places[d, far % DIMS[d]]

    def slot(self, cls):
        d1, d2, d3 = ORDER[cls]
        return (self.at[d1] * DIMS[d2] + self.at[d2]) * DIMS[d3] + self.at[d3]


def greet(peers):
    barrier = pltpu.get_barrier_semaphore()
    for peer in peers:
        pl.semaphore_signal(barrier, inc=1, device_id=peer)
    pl.semaphore_wait(barrier, len(peers))


def line_peers(me):
    return [me.beside(d, s) for d, n in DIMS.items() for s in range(1, n)]


def chain(n):
    half = n // PAIR
    stages = []
    for i in range(1, half + 1):
        far = half - i + 1
        now = [(1, far, None if i == 1 else i - PAIR, i - 1)]
        if i >= PAIR:
            now.append((-1, far, None if i == PAIR else half + i - 3, half + i - PAIR))
        stages.append(now)
    return stages, [half - 1] + ([n - PAIR] if half >= PAIR else [])


def arrived(ref, sem):
    pltpu.make_async_copy(ref, ref, sem).wait()


class Reduce:
    def __init__(self, me, d, sign, own_at, send_at, recv_at, size, sent, came, step, raw):
        self.me, self.d, self.sign, self.n = me, d, sign, DIMS[d]
        self.own_at, self.send_at, self.recv_at = own_at, send_at, recv_at
        self.size, self.sent, self.came, self.step, self.raw = size, sent, came, min(step, size), raw
        self.stages, self.last = chain(self.n)

    def each(self, body):
        if self.size == self.step:
            body(0)
        else:
            lax.fori_loop(0, self.size // self.step, lambda i, _: body(i * self.step), None)

    def go(self, stage):
        if stage > 0:
            arrived(self.recv_at(0, 0, self.size, len(self.stages[stage - 1])), self.came(stage - 1))
        if stage == len(self.stages):
            return
        for way, far, joins, into in self.stages[stage]:
            block = self.me.block(self.d, self.sign * way * far)
            if joins is not None or not self.raw:
                def body(first):
                    v = self.own_at(block, first, self.step)[...].astype(F32)
                    if joins is not None:
                        v = v + self.recv_at(joins, first, self.step, 1)[0].astype(F32)
                    self.send_at(block, first, self.step)[...] = v.astype(BF16)
                self.each(body)
            pltpu.make_async_remote_copy(self.send_at(block, 0, self.size), self.recv_at(into, 0, self.size, 1).at[0], self.sent, self.came(stage),
                                         device_id=self.me.beside(self.d, self.sign * way)).start()

    def finish(self, put):
        def body(first):
            v = self.own_at(self.me.at[self.d], first, self.step)[...].astype(F32)
            for r in self.last:
                v = v + self.recv_at(r, first, self.step, 1)[0].astype(F32)
            put(first, self.step, v)
        self.each(body)

    def drain(self):
        arrived(self.send_at(0, 0, self.size * (self.n - 1)), self.sent)


class DirectReduce:
    stages = (None,)

    def __init__(self, me, d, own_at, send_at, recv_at, sent, came):
        self.me, self.d, self.n = me, d, DIMS[d]
        self.own_at, self.send_at, self.recv_at, self.sent, self.came = own_at, send_at, recv_at, sent, came

    def go(self, stage):
        if stage == 1:
            arrived(self.recv_at(0, 0, 1, self.n - 1), self.came(0))
            return
        for far in range(1, self.n):
            block = self.send_at(self.me.block(self.d, far), 0, 1)
            block[...] = self.own_at(self.me.block(self.d, far), 0, 1)[...].astype(BF16)
            pltpu.make_async_remote_copy(block, self.recv_at(far - 1, 0, 1, 1).at[0], self.sent, self.came(0), device_id=self.me.beside(self.d, far)).start()

    def finish(self, put):
        v = self.own_at(self.me.at[self.d], 0, 1)[...].astype(F32)
        for far in range(self.n - 1):
            v = v + self.recv_at(far, 0, 1, 1)[0].astype(F32)
        put(0, 1, v)

    def drain(self):
        arrived(self.send_at(0, 0, self.n - 1), self.sent)


class Gather:
    def __init__(self, me, d, sign, at, sent, came):
        self.me, self.d, self.sign, self.n, self.at, self.sent, self.came = me, d, sign, DIMS[d], at, sent, came
        half = self.n // PAIR
        self.stages = [[way for way in (1, -1) if stage < half or way == sign] for stage in range(1, half + 1)]

    def go(self, stage):
        if stage > 0:
            arrived(self.at(0, len(self.stages[stage - 1])), self.came(stage - 1))
        if stage < len(self.stages):
            for way in self.stages[stage]:
                block = self.at(self.me.block(self.d, -way * stage), 1)
                pltpu.make_async_remote_copy(block, block, self.sent, self.came(stage), device_id=self.me.beside(self.d, way)).start()

    def drain(self):
        arrived(self.at(0, self.n - 1), self.sent)


class DirectGather:
    stages = (None,)

    def __init__(self, me, d, at, sent, came):
        self.me, self.d, self.n, self.at, self.sent, self.came = me, d, DIMS[d], at, sent, came

    def go(self, stage):
        if stage == 1:
            arrived(self.at(0, self.n - 1), self.came(0))
            return
        block = self.at(self.me.at[self.d], 1)
        for far in range(1, self.n):
            pltpu.make_async_remote_copy(block, block, self.sent, self.came(0), device_id=self.me.beside(self.d, far)).start()

    def drain(self):
        arrived(self.at(0, self.n - 1), self.sent)


class GroupSum:
    def __init__(self, me, ref, sent, came):
        self.me, self.ref, self.sent, self.came = me, ref, sent, came
        self.names = list(DIMS)

    def ring(self, n):
        return DirectGather(self.me, self.names[n], lambda i, many: self.ref.at[n, pl.ds(i, many)], self.sent.at[n], lambda stage: self.came.at[n])

    def go(self, n):
        if n > 0:
            before = self.ring(n - 1)
            before.go(1)
            total = self.ref[n - 1, 0]
            for i in range(1, before.n):
                total = total + self.ref[n - 1, i]
            to = self.me.at[self.names[n]] if n < len(self.names) else 0
            self.ref[n, pl.ds(to, 1)] = total[None]
            before.drain()
        if n < len(self.names):
            self.ring(n).go(0)


STAGES = 4


class Reduction:
    def __init__(self, me, tb, rx, left, sent, came):
        self.me, self.tb, self.rx, self.left, self.sent, self.came = me, tb, rx, left, sent, came

    def step(self, wave, slot, event):
        for c, (cls, sign, _) in enumerate(SETS):
            n1, n2, n3 = sizes(cls)
            size = n2 * n3
            pace = 4 // (n1 // PAIR)
            if event % pace == 0:
                own = lambda block, first, step: self.tb[c].at[slot, pl.ds(block * size + first, step)]
                ring = Reduce(self.me, ORDER[cls][0], sign, own, own, lambda i, first, step, many: self.rx[c].at[wave, pl.ds(i, many), pl.ds(first, step)], size,
                              self.sent.at[wave, c], lambda stage: self.came.at[wave, c, stage], SUB, True)
                ring.go(event // pace)
                if event == 4:
                    def put(first, step, v):
                        self.left[c][wave, pl.ds(first, step)] = v
                    ring.finish(put)
                    ring.drain()


class Late:
    def __init__(self, me, left, refs, put, direct):
        send2, rx2, acc3, send3, rx3, (sent, came) = deal(refs, NSETS, NSETS, NSETS, NSETS, NSETS)
        self.acc3, self.put, self.rings = acc3, put, []
        for c, (cls, sign, _) in enumerate(SETS):
            self.rings.append(self.of(me, cls, sign, left[c], send2[c], rx2[c], acc3[c], send3[c], rx3[c], sent.at[0, c], sent.at[1, c],
                                      functools.partial(lambda c, ring, stage: came.at[ring, c, stage], c), direct))
        self.last = max(len(two.stages) + len(three.stages) for two, three in self.rings)

    @staticmethod
    def of(me, cls, sign, left, send2, rx2, acc3, send3, rx3, sent2, sent3, came, direct):
        _, d2, d3 = ORDER[cls]
        n3 = DIMS[d3]
        two = Reduce(me, d2, sign, lambda b, f, st: left.at[:, pl.ds(b * n3 + f, st)], lambda b, f, st: send2.at[:, pl.ds(b * n3 + f, st)],
                     lambda i, f, st, many: rx2.at[pl.ds(i, many), :, pl.ds(f, st)], n3, sent2, functools.partial(came, 0), 4, False)
        at3 = (lambda b, f, st: acc3.at[:, pl.ds(b + f, st)], lambda b, f, st: send3.at[:, pl.ds(b + f, st)], lambda i, f, st, many: rx3.at[pl.ds(i, many)])
        if direct:
            return two, DirectReduce(me, d3, *at3, sent3, functools.partial(came, 1))
        return two, Reduce(me, d3, sign, *at3, 1, sent3, functools.partial(came, 1), 1, False)

    def go(self, event):
        for c, (two, three) in enumerate(self.rings):
            half = len(two.stages)
            if event <= half:
                two.go(event)
            if event == half:
                def put3(first, step, v):
                    self.acc3[c][:, pl.ds(first, step)] = v
                two.finish(put3)
            if half <= event <= half + len(three.stages):
                three.go(event - half)
            if event == half + len(three.stages):
                three.finish(lambda first, step, v: self.put(c, v[:, 0]))
                two.drain()
                three.drain()


def late_buffers(waves):
    made = [[] for _ in range(5)]
    for cls, _, k in SETS:
        n1, n2, n3 = sizes(cls)
        for to, shape, dtype in zip(made, ((waves, n2 * n3), (n2 - 1, waves, n3), (waves, n3), (waves, n3), (n3 - 1, waves, 1)), (BF16, BF16, F32, BF16, BF16)):
            to.append(vm((*shape, k, SUB, LANES), dtype))
    return sum(made, []) + light_sems()


def semaphores(*shapes):
    return [pltpu.SemaphoreType.DMA(shape) for shape in shapes]


def reduction_buffers(slots, waves):
    tb, rx = [], []
    for cls, _, k in SETS:
        n1, n2, n3 = sizes(cls)
        tb.append(vm((slots, devices(), k, SUB, LANES), BF16))
        rx.append(vm((waves, n1 - 1, n2 * n3, k, SUB, LANES), BF16))
    return [*tb, *rx, *semaphores((waves, NSETS), (waves, NSETS, STAGES))]


class LightGather:
    def __init__(self, me, at, sent, came, direct):
        self.rings = [self.of(me, cls, sign, functools.partial(at, c), sent.at[0, c], sent.at[1, c],
                              functools.partial(lambda c, ring, stage: came.at[ring, c, stage], c), direct) for c, (cls, sign, _) in enumerate(SETS)]
        self.last = max(len(three.stages) + len(two.stages) for three, two in self.rings)

    @staticmethod
    def of(me, cls, sign, at, sent2, sent3, came, direct):
        _, d2, d3 = ORDER[cls]
        n3 = DIMS[d3]
        at3 = lambda i, many: at(me.at[d2] * n3 + i, many)
        if direct:
            three = DirectGather(me, d3, at3, sent3, functools.partial(came, 1))
        else:
            three = Gather(me, d3, sign, at3, sent3, functools.partial(came, 1))
        return three, Gather(me, d2, sign, lambda i, many: at(i * n3, many * n3), sent2, functools.partial(came, 0))

    def go(self, event):
        for three, two in self.rings:
            first = len(three.stages)
            if event <= first:
                three.go(event)
            if first <= event <= first + len(two.stages):
                two.go(event - first)
            if event == first + len(two.stages):
                three.drain()
                two.drain()


def light_sems():
    return semaphores((PAIR, NSETS), (PAIR, NSETS, STAGES))


FFN_WAVES, OWN_WAVES = STRIPES, PAIR


def left_shapes():
    return [(FFN_WAVES, sizes(cls)[1] * sizes(cls)[PAIR], k, SUB, LANES) for cls, _, k in SETS]


def reduce_loop(waves, reduction, slots, pieces):
    def body(i, _):
        for p, piece in enumerate(pieces):
            for event in reversed(range(5)):
                back = p - PAIR - PAIR * event
                if back % len(pieces) == 0:
                    w = i + back // len(pieces)

                    @pl.when((w >= 0) & (w < waves))
                    def _():
                        reduction.step(w, w % slots, event)

            @pl.when(i < waves)
            def _():
                piece(i)

    lax.fori_loop(0, waves + 3, body, None)


FF_CHUNK = 512
TOKEN_BLOCK = 512


def ffn_kernel(waves, x_ref, dy_ref, wg_ref, wu_ref, wd_ref, *refs):
    left, (db_ref, *refs) = deal(refs, NSETS)
    tb, rx, (sent, came, *rest) = deal(refs, NSETS, NSETS)
    wbuf, wdbuf, hid_s, dg_s, du_s, dbg, dbu, wsem = rest
    me = Place()
    slots = tb[0].shape[0]

    def weights(j, s):
        cols = pl.ds(pl.multiple_of(j * FF_CHUNK, FF_CHUNK), FF_CHUNK)
        return [pltpu.make_async_copy(wg_ref.at[0, :, cols], wbuf.at[s, 0], wsem.at[s, 0]),
                pltpu.make_async_copy(wu_ref.at[0, :, cols], wbuf.at[s, 1], wsem.at[s, 1]),
                pltpu.make_async_copy(wd_ref.at[0, cols, :], wdbuf.at[s], wsem.at[s, PAIR])]

    for copy in weights(0, 0):
        copy.start()
    dbg[...] = jnp.zeros_like(dbg)
    dbu[...] = jnp.zeros_like(dbu)
    pad_c, pad_k = WAVE[10]
    for s in range(slots):
        tb[pad_c][s, devices() // PAIR:, pad_k] = jnp.zeros((devices() // PAIR, SUB, LANES), BF16)
    greet(line_peers(me))

    def hidden_units(j):
        s = j % PAIR
        for copy in weights(j, s):
            copy.wait()

        @pl.when(j + 1 < waves)
        def _():
            for copy in weights(j + 1, 1 - s):
                copy.start()

        def tokens(n, _):
            rows = pl.ds(pl.multiple_of(n * TOKEN_BLOCK, TOKEN_BLOCK), TOKEN_BLOCK)
            b = x_ref[rows, :]
            gate = _dot(b, wbuf[s, 0], 1, 0)
            up = _dot(b, wbuf[s, 1], 1, 0)
            dh = _dot(dy_ref[rows, :], wdbuf[s], 1, 1).astype(BF16).astype(F32)
            sig = 1.0 / (1.0 + jnp.exp(-gate))
            silu = gate * sig
            hid_s[rows, :] = (silu * up).astype(BF16)
            du_s[rows, :] = (dh * silu).astype(BF16)
            dg_s[rows, :] = (dh * up * (sig + silu * (1.0 - sig))).astype(BF16)

        lax.fori_loop(0, x_ref.shape[0] // TOKEN_BLOCK, tokens, None)

    def by_weights(j):
        slot = j % slots
        for half, src in enumerate((dg_s, du_s)):
            g = _dot(x_ref[...], src[...], 0, 0).astype(BF16)
            for t in range(STRIPES):
                c, k = WAVE[t]
                for i in range(4):
                    tb[c][slot, pl.ds(HALF_PART * half + TILE * i, TILE), k] = g[LANES * t : LANES * t + LANES, LANES * i : LANES * i + LANES].reshape(TILE, SUB, LANES)
        g = _dot(hid_s[...], dy_ref[...], 0, 0).astype(BF16)
        for i in range(STRIPES):
            c, k = WAVE[STRIPES + i // PAIR]
            tb[c][slot, pl.ds(HALF_PART * (i % PAIR), HALF_PART), k] = g[:, LANES * i : LANES * i + LANES].reshape(HALF_PART, SUB, LANES)

    def by_input(j):
        for n, (to, src) in enumerate(((dbg, dg_s), (dbu, du_s))):
            to[...] += _dot(src[...], wbuf[j % PAIR, n], 1, 1)

    reduce_loop(waves, Reduction(me, tb, rx, left, sent, came), slots, (hidden_units, by_weights, by_input))
    db_ref[...] = (dbg[...].astype(BF16).astype(F32) + dbu[...].astype(BF16).astype(F32)).astype(BF16)


def ffn_call(b, dy, wg, wu, wd):
    waves = wg.shape[PAIR] // FF_CHUNK
    tokens, d = b.shape
    whole = pl.BlockSpec(memory_space=pltpu.VMEM)
    anywhere = pl.BlockSpec(memory_space=pl.ANY)
    mid = vm((tokens, FF_CHUNK), BF16)
    left = [vm(s, F32) for s in left_shapes()]
    return pl.pallas_call(
        functools.partial(ffn_kernel, waves),
        out_shape=left + [jax.ShapeDtypeStruct((tokens, d), BF16)],
        in_specs=[whole, whole, anywhere, anywhere, anywhere],
        out_specs=[whole] * STRIPES,
        scratch_shapes=reduction_buffers(3, waves) + [
            vm((PAIR, PAIR, d, FF_CHUNK), BF16), vm((PAIR, FF_CHUNK, d), BF16), mid, mid, mid, vm((tokens, d), F32), vm((tokens, d), F32),
            pltpu.SemaphoreType.DMA((PAIR, 3))],
        compiler_params=pltpu.CompilerParams(collective_id=0, has_side_effects=True, vmem_limit_bytes=room(*left)),
        cost_estimate=pl.CostEstimate(flops=TILE * tokens * d * wg.shape[PAIR], transcendentals=tokens * wg.shape[PAIR], bytes_accessed=40_000_000),
    )(b, dy, wg, wu, wd)


def share_slot(me, cls):
    d1, d2, d3 = ORDER[cls]
    return me.at[d2] * DIMS[d3] + me.at[d3]


def gather_kernel(*refs):
    shares, tb_in, moments, g, (tot_out, *refs) = deal(refs, NSETS, NSETS, len(AHEAD), NSETS)
    ahead, refs = deal(refs, len(AHEAD))
    tb, rx, left, (sent, came, *refs) = deal(refs, NSETS, NSETS, NSETS)
    late, (nrm, lsem, msem, ns, nr, g1s, g1r, *light) = deal(refs, len(refs) - 11)
    me = Place()
    waves = FFN_WAVES + OWN_WAVES

    loads = [pltpu.make_async_copy(tb_in[c], tb[c], lsem.at[c]) for c in range(NSETS)]
    fetched = [pltpu.make_async_copy(src, to, msem.at[n]) for n, (src, to) in enumerate(zip(moments, ahead))]
    for copy in loads + fetched:
        copy.start()
    for c, (cls, _, _) in enumerate(SETS):
        g[c][:FFN_WAVES, me.slot(cls)] = shares[c][...]
    greet(line_peers(me))
    for copy in loads:
        copy.wait()

    def put(c, v):
        g[c][FFN_WAVES:, me.slot(SETS[c][0])] = v.astype(BF16)

    def block(first_wave, count):
        def at(c, first, size):
            cls, _, _ = SETS[c]
            _, n2, n3 = sizes(cls)
            return g[c].at[pl.ds(first_wave, count), pl.ds(me.at[ORDER[cls][0]] * n2 * n3 + first, size)]
        return at

    reduction = Reduction(me, tb, rx, left, sent, came)
    rest = Late(me, left, late, put, True)
    summing = GroupSum(me, nrm, ns, nr)
    spread_ffn = LightGather(me, block(0, FFN_WAVES), *light[:PAIR], False)
    spread = LightGather(me, block(FFN_WAVES, OWN_WAVES), *light[PAIR:], True)

    def norm():
        total = jnp.zeros((SUB, LANES), F32)
        for c, (cls, _, _) in enumerate(SETS):
            v = g[c][:, me.slot(cls)].astype(F32)
            total = total + jnp.sum(v * v, axis=(0, 1))
        nrm[0, pl.ds(me.at["x"], 1)] = total[None]

    ready = 4 + rest.last

    def chain(point):
        if point < 5:
            for w in range(OWN_WAVES):
                reduction.step(w, w, point)
        if point <= spread_ffn.last:
            spread_ffn.go(point)
        if 4 <= point <= ready:
            rest.go(point - 4)
        if point == ready:
            norm()
        if ready <= point <= ready + max(spread.last, len(DIMS)):
            if point - ready <= spread.last:
                spread.go(point - ready)
            if point - ready <= len(DIMS):
                summing.go(point - ready)

    def far(wave, event):
        for c, (cls, sign, _) in enumerate(SETS):
            n1, n2, n3 = sizes(cls)
            pace = 4 // (n1 // PAIR)
            if event % pace == 0:
                size = n2 * n3
                ring = Gather(me, ORDER[cls][0], sign, lambda i, many: g[c].at[wave, pl.ds(i * size, many * size)], g1s.at[wave, c],
                              lambda stage: g1r.at[wave, c, stage])
                ring.go(event // pace)
                if event == 4:
                    ring.drain()

    begin = spread_ffn.last // PAIR

    def body(i, _):
        for half in range(PAIR):
            for point in range(half, ready + 1 + max(spread.last, len(DIMS)), PAIR):
                @pl.when(i == point // PAIR)
                def _():
                    chain(point)
            for event in reversed(range(half, 5, PAIR)):
                w = i - event - begin

                @pl.when((w >= 0) & (w < waves))
                def _():
                    far(w, event)

    lax.fori_loop(0, waves + 4 + begin, body, None)
    tot_out[...] = nrm[len(DIMS), 0]
    for copy in fetched:
        copy.wait()


AHEAD = (0, 3, 1)
AHEAD = tuple((kind, n) for n in AHEAD for kind in (0, 1))


def gather_call(shares, own, moments):
    waves = FFN_WAVES + OWN_WAVES
    whole = pl.BlockSpec(memory_space=pltpu.VMEM)
    anywhere = pl.BlockSpec(memory_space=pl.ANY)
    left = [vm((OWN_WAVES, *s[1:]), F32) for s in left_shapes()]
    buffers, sems = deal(reduction_buffers(OWN_WAVES, OWN_WAVES), 12)
    kept = [vm((waves, devices(), k, SUB, LANES), BF16) for _, _, k in SETS] + [vm((SUB, LANES), F32)] + [vm(a.shape, F32) for a in moments]
    return pl.pallas_call(
        gather_kernel,
        out_shape=kept,
        in_specs=[whole] * NSETS + [anywhere] * (NSETS + len(moments)),
        out_specs=[whole] * (STRIPES + len(moments)),
        scratch_shapes=buffers + left + sems + late_buffers(OWN_WAVES) + [vm((4, SUB, SUB, LANES), F32)]
        + semaphores((NSETS,), (len(moments),), (len(DIMS),), (len(DIMS),), (waves, NSETS), (waves, NSETS, STAGES)) + light_sems() + light_sems(),
        compiler_params=pltpu.CompilerParams(collective_id=1, has_side_effects=True, vmem_limit_bytes=room(*kept)),
        cost_estimate=pl.CostEstimate(flops=10_000_000_000, transcendentals=0, bytes_accessed=60_000_000),
    )(*shares, *own, *moments)


COUNT = 12386304


def attention_parts():
    return [(kind, t) for kind in ("o", "kv", "q") for t in range(STRIPES)]


def place_of(kind, j, t):
    if kind in ("gu", "d"):
        c, k = WAVE[t if kind == "gu" else STRIPES + t]
        return c, j, k
    n = attention_parts().index((kind, t))
    c, k = WAVE[n % 11]
    return c, FFN_WAVES + n // 11, k


def adam_job(kind, j, n):
    if kind in ("gu", "q", "kv"):
        rows = LANES * n
        col = pl.multiple_of(512 * j, 512) if kind == "gu" else 0
        pieces = {"gu": [(4, rows, col, 512, 0), (5, rows, col, 512, 512)], "q": [(0, rows, 0, 1024, 0)], "kv": [(1, rows, 0, 512, 0), (PAIR, rows, 0, 512, 512)]}
        return pieces[kind], [(*place_of(kind, j, n), TILE * i) for i in range(SUB)]
    if kind == "o":
        return [(3, LANES * n, 0, 896, 0)], [(*place_of(kind, j, t), TILE * n) for t in range(STRIPES)]
    row = pl.multiple_of(512 * j + LANES * n, LANES)
    return [(NSETS, row, 0, 896, 0)], [(*place_of(kind, j, t // PAIR), HALF_PART * (t % PAIR) + TILE * n) for t in range(STRIPES)]


ROUND = [("gu", n) for n in range(STRIPES)] + [("d", n) for n in range(4)]
REST = [("o", n) for n in range(SUB)] + [(kind, n) for kind in ("kv", "q") for n in range(STRIPES)]


def adam_kernel(depth, *refs):
    n = len(NAMES)
    w, m, v, (tot, *refs) = deal(refs, n, n, n)
    g, held, wo, mo, vo, rest = deal(refs, NSETS, len(AHEAD), n, n, n)
    wb, mb, vb, wn, mn, vn, isem, osem = rest
    ahead, period = depth - 1, len(ROUND)

    def moves(job, s, out):
        made = []
        for n, (which, row, col, width, at) in enumerate(job[0]):
            for a, (old, new, near, late) in enumerate(((w, wo, wb, wn), (m, mo, mb, mn), (v, vo, vb, vn))):
                if not out and (a - 1, which) in AHEAD:
                    continue
                far = (new if out else old)[which].at[0, pl.ds(row, LANES), pl.ds(col, width)]
                here = (late if out else near).at[s, :, pl.ds(at, width)]
                made.append(pltpu.make_async_copy(here, far, osem.at[s, n, a]) if out else pltpu.make_async_copy(far, here, isem.at[s, n, a]))
        return made

    def start(job, s, out):
        for copy in moves(job, s, out):
            copy.start()

    def finish(job, s, out):
        for copy in moves(job, s, out):
            copy.wait()

    def work(job, s):
        def body(r, _):
            rows = pl.ds(pl.multiple_of(TILE * r, TILE), TILE)

            def moment(kind, n, buf):
                which, row, _, width, at = [p for p in job[0] if p[4] <= LANES * n][-1]
                if (kind, which) in AHEAD:
                    return held[AHEAD.index((kind, which))][0, pl.ds(pl.multiple_of(row + TILE * r, TILE), TILE), LANES * n - at : LANES * n - at + LANES]
                return buf[s, rows, LANES * n : LANES * n + LANES]

            for n, (c, wave, k, slot) in enumerate(job[1]):
                cols = slice(LANES * n, LANES * n + LANES)
                x = g[c][wave, pl.ds(slot + PAIR * r, PAIR), k].astype(F32).reshape(TILE, LANES) * factor
                a = 0.9 * moment(0, n, mb) + 0.1 * x
                b = 0.95 * moment(1, n, vb) + 0.05 * x * x
                old = wb[s, rows, cols].astype(F32)
                mn[s, rows, cols] = a
                vn[s, rows, cols] = b
                wn[s, rows, cols] = (old - 0.02 * (a * lax.rsqrt(b + 1e-8) + 0.1 * old)).astype(BF16)

        lax.fori_loop(0, SUB, body, None)

    for i in range(ahead):
        start(adam_job(*(ROUND[i][0], 0, ROUND[i][1])), i, False)
    square = jnp.sum(tot[...], keepdims=True)
    factor = jnp.broadcast_to(jnp.minimum(1.0, 0.5 * lax.rsqrt(square / COUNT + 1e-30)), (TILE, LANES))
    job_of = lambda i, j: adam_job(ROUND[i][0], j, ROUND[i][1])
    rest_job = lambda i: adam_job(REST[i][0], 0, REST[i][1])

    def chunk(j, _):
        for i in range(period):
            at = period * j + i
            s = lax.rem(at, depth)
            nxt = lax.rem(at + ahead, depth)
            if i + ahead < period:
                start(job_of(i + ahead, j), nxt, False)
            else:
                later = i + ahead - period

                @pl.when(j + 1 < FFN_WAVES)
                def _():
                    start(job_of(later, j + 1), nxt, False)

                @pl.when(j + 1 == FFN_WAVES)
                def _():
                    start(rest_job(later), nxt, False)
            finish(job_of(i, j), s, False)
            if i >= depth:
                finish(job_of(i - depth, j), s, True)
            else:
                @pl.when(j > 0)
                def _():
                    finish(job_of(i - depth + period, j - 1), s, True)
            work(job_of(i, j), s)
            start(job_of(i, j), s, True)

    lax.fori_loop(0, FFN_WAVES, chunk, None)
    base = period * FFN_WAVES
    for i in range(len(REST)):
        s = (base + i) % depth
        if i + ahead < len(REST):
            start(rest_job(i + ahead), (base + i + ahead) % depth, False)
        finish(rest_job(i), s, False)
        finish(rest_job(i - depth) if i >= depth else job_of(i - depth + period, FFN_WAVES - 1), s, True)
        work(rest_job(i), s)
        start(rest_job(i), s, True)
    for i in range(len(REST) - depth, len(REST)):
        finish(rest_job(i), (base + i) % depth, True)


def adam_call(w, m, v, tot, gs, ahead, depth=4):
    anywhere = pl.BlockSpec(memory_space=pl.ANY)
    whole = pl.BlockSpec(memory_space=pltpu.VMEM)
    buf = lambda t: vm((depth, LANES, 1024), t)
    dma = pltpu.SemaphoreType.DMA
    return pl.pallas_call(
        functools.partial(adam_kernel, depth),
        out_shape=[jax.ShapeDtypeStruct(x.shape, x.dtype) for x in (*w, *m, *v)],
        in_specs=[anywhere] * 21 + [whole] * (STRIPES + len(ahead)),
        out_specs=[anywhere] * 21,
        scratch_shapes=[buf(BF16), buf(F32), buf(F32)] * PAIR + [dma((depth, PAIR, 3))] * PAIR,
        compiler_params=pltpu.CompilerParams(vmem_limit_bytes=room(tot, *gs, *ahead)),
        cost_estimate=pl.CostEstimate(flops=25 * COUNT, transcendentals=COUNT, bytes_accessed=270_000_000),
    )(*w, *m, *v, *in_vmem([tot, *gs, *ahead]))


HEAD, GROUPS, PER = 256, PAIR, PAIR
QB = 256
LOG2E = 1.4426950408889634


def _dot(a, b, ca, cb):
    return lax.dot_general(a, b, (((ca,), (cb,)), ((), ())), preferred_element_type=F32)


def root(wide):
    return lax.rsqrt(jnp.mean(wide * wide, -1, keepdims=True) + 1e-6)


def turn(t, cos, sin):
    a, b = t[:, : HEAD // PAIR], t[:, HEAD // PAIR :]
    return jnp.concatenate([a * cos - b * sin, b * cos + a * sin], -1)


def head(g, h):
    return pl.ds(pl.multiple_of((PER * g + h) * HEAD, HEAD), HEAD)


def stacked(ref, rows, g):
    return jnp.concatenate([ref[rows, head(g, h)] for h in range(PER)], 0)


def hidden(s, fill):
    n = s.shape[0]
    own = s[n - QB :]
    key = lax.broadcasted_iota(jnp.int32, own.shape, 0)
    query = lax.broadcasted_iota(jnp.int32, own.shape, 1) % QB
    own = jnp.where(key <= query, own, fill)
    return own if n == QB else jnp.concatenate([s[: n - QB], own], 0)


def forward_kernel(x, wq, wk, wv, wo, far, near, a_o, q_o, k_o, v_o, out_o, lse_o, h_o, b_o, cos, sin):
    tokens = x.shape[0]
    big = 512
    some = near.shape[1]

    def angles(n, _):
        rows = pl.ds(pl.multiple_of(n * some, some), some)
        c, s = far[0, pl.ds(n, 1)], far[1, pl.ds(n, 1)]
        cos[rows, :] = c * near[0] - s * near[1]
        sin[rows, :] = s * near[0] + c * near[1]

    lax.fori_loop(0, tokens // some, angles, None)

    def project(n, _):
        rows = pl.ds(pl.multiple_of(n * big, big), big)
        wide = x[rows, :].astype(F32)
        a = (wide * root(wide)).astype(BF16)
        a_o[rows, :] = a
        c, s = cos[rows, :], sin[rows, :]
        for w, to in ((wq, q_o), (wk, k_o)):
            t = _dot(a, w[0], 1, 0).astype(BF16).astype(F32)
            for at in range(0, t.shape[1], HEAD):
                to[rows, at : at + HEAD] = turn(t[:, at : at + HEAD], c, s).astype(BF16)
        v_o[rows, :] = _dot(a, wv[0], 1, 0).astype(BF16)

    lax.fori_loop(0, tokens // big, project, None)
    e = HEAD**-0.5 * LOG2E

    def attend(g, _):
        cols = pl.ds(pl.multiple_of(g * HEAD, HEAD), HEAD)
        for i in range(tokens // QB):
            rows, n = slice(QB * i, QB * i + QB), QB * (i + 1)
            s = hidden(_dot(k_o[:n, cols], stacked(q_o, rows, g), 1, 1), -1e30)
            top = s.max(0, keepdims=True)
            p = jnp.exp2((s - top) * e)
            total = p.sum(0, keepdims=True)
            p = (p * (1.0 / total)).astype(BF16)
            out = _dot(v_o[:n, cols], p, 0, 0).T.astype(BF16)
            lse = top * e + jnp.log2(total)
            for h in range(PER):
                out_o[rows, head(g, h)] = out[QB * h : QB * h + QB]
                lse_o[g, h : h + 1, rows] = lse[:, QB * h : QB * h + QB]

    lax.fori_loop(0, GROUPS, attend, None)

    def finish(n, _):
        rows = pl.ds(pl.multiple_of(n * big, big), big)
        h = (x[rows, :].astype(F32) + _dot(out_o[rows, :], wo[0], 1, 0).astype(BF16).astype(F32)).astype(BF16)
        h_o[rows, :] = h
        wide = h.astype(F32)
        b_o[rows, :] = (wide * root(wide)).astype(BF16)

    lax.fori_loop(0, tokens // big, finish, None)


def forward_call(x, wq, wk, wv, wo, far, near):
    tokens, d = x.shape
    out = lambda n: jax.ShapeDtypeStruct((tokens, n), BF16)
    nq, nk = wq.shape[PAIR], wk.shape[PAIR]
    whole = pl.BlockSpec(memory_space=pltpu.VMEM)
    return pl.pallas_call(
        forward_kernel,
        out_shape=[out(d), out(nq), out(nk), out(nk), out(nq), jax.ShapeDtypeStruct((GROUPS, PER, tokens), F32), out(d), out(d)]
        + [jax.ShapeDtypeStruct((tokens, HEAD // PAIR), F32)] * PAIR,
        in_specs=[whole] * STRIPES,
        out_specs=[whole] * 10,
        compiler_params=pltpu.CompilerParams(vmem_limit_bytes=VM),
        cost_estimate=pl.CostEstimate(flops=12_000_000_000, transcendentals=4_000_000, bytes_accessed=25_000_000),
    )(x, wq, wk, wv, wo, far, near)


def own_place(kind, t):
    c, wave, k = place_of(kind, 0, t)
    return c, wave - FFN_WAVES, k


def backward_pieces(refs):
    r = refs
    tokens = r.dy.shape[0]
    big = 512
    e, scale = HEAD**-0.5 * LOG2E, HEAD**-0.5

    def by_norm():
        def body(n, _):
            rows = pl.ds(pl.multiple_of(n * big, big), big)
            wide = r.h[rows, :].astype(F32)
            by = r.by_b[rows, :].astype(F32)
            s = root(wide)
            back = by * s - wide * (s * s * s * jnp.mean(by * wide, -1, keepdims=True))
            r.by_h[rows, :] = (r.dy[rows, :].astype(F32) + back.astype(BF16).astype(F32)).astype(BF16)
            r.by_out[rows, :] = _dot(r.by_h[rows, :], r.wo[0], 1, 1).astype(BF16)

        lax.fori_loop(0, tokens // big, body, None)

    def by_wo():
        g = _dot(r.out[...], r.by_h[...], 0, 0).astype(BF16)
        for t in range(STRIPES):
            c, w, k = own_place("o", t)
            r.own[c][w, :, k] = g[:, LANES * t : LANES * t + LANES].reshape(devices(), SUB, LANES)

    def attend(i):
        rows, n = slice(QB * i, QB * i + QB), QB * (i + 1)

        def body(g, _):
            cols = pl.ds(pl.multiple_of(g * HEAD, HEAD), HEAD)
            q, do = stacked(r.q, rows, g), stacked(r.by_out, rows, g)
            lse = jnp.concatenate([r.lse[g, h : h + 1, rows] for h in range(PER)], 1)
            p = hidden(jnp.exp2(_dot(r.k[:n, cols], q, 1, 1) * e - lse), 0.0)
            dp = _dot(r.v[:n, cols], do, 1, 1)
            delta = (p * dp).sum(0, keepdims=True)
            ds = (p * (dp - delta)).astype(BF16)
            r.by_v[:n, cols] += _dot(p.astype(BF16), do, 1, 0)
            r.by_k[:n, cols] += _dot(ds, q, 1, 0)
            dq = (_dot(r.k[:n, cols], ds, 0, 0) * scale).T.astype(BF16).astype(F32)
            for h in range(PER):
                r.by_q[rows, head(g, h)] = turn(dq[QB * h : QB * h + QB], r.cos[rows, :], -r.sin[rows, :]).astype(BF16)

        return lambda: lax.fori_loop(0, GROUPS, body, None)

    def clear():
        r.by_k[...] = jnp.zeros_like(r.by_k)
        r.by_v[...] = jnp.zeros_like(r.by_v)

    def by_w(kind, first, source):
        g = _dot(r.a[...], source, 0, 0).astype(BF16)
        for t in range(STRIPES):
            c, w, k = own_place(kind, t)
            for n in range(4):
                r.own[c][w, pl.ds(TILE * (first + n), TILE), k] = g[LANES * t : LANES * t + LANES, LANES * n : LANES * n + LANES].reshape(TILE, SUB, LANES)

    def by_keys():
        by_w("kv", 0, jnp.concatenate([turn((r.by_k[:, HEAD * g : HEAD * g + HEAD] * scale).astype(BF16).astype(F32), r.cos[...], -r.sin[...]).astype(BF16)
                                       for g in range(GROUPS)], 1))

    def by_queries():
        lax.fori_loop(0, PAIR, lambda n, _: by_w("q", 4 * n, r.by_q[:, pl.ds(pl.multiple_of(512 * n, 512), 512)]), None)

    return [clear, by_norm, by_wo, *(attend(i) for i in range(tokens // QB)), lambda: by_w("kv", 4, r.by_v[...].astype(BF16)), by_keys, by_queries]


class Names:
    def __init__(self, **refs):
        self.__dict__.update(refs)


BACKWARD = ("dy", "h", "by_b", "a", "q", "k", "v", "out", "lse", "wo", "cos", "sin")
BACKWARD_SCRATCH = ("by_h", "by_out", "by_q", "by_k", "by_v")


def backward_scratch(tokens, d):
    wide, key = GROUPS * PER * HEAD, GROUPS * HEAD
    return [vm((tokens, d), BF16), vm((tokens, wide), BF16), vm((tokens, wide), BF16), vm((tokens, key), F32), vm((tokens, key), F32)]


def backward_kernel(*refs):
    given, left, shares, own, refs = deal(refs, len(BACKWARD), NSETS, NSETS, NSETS)
    buffers, refs = deal(refs, len(BACKWARD_SCRATCH))
    me = Place()

    def put(c, v):
        shares[c][...] = v.astype(BF16)

    pad, k = WAVE[10]
    own[pad][OWN_WAVES - 1, :, k] = jnp.zeros((devices(), SUB, LANES), BF16)
    greet(line_peers(me))
    rest = Late(me, left, refs, put, False)
    pieces = backward_pieces(Names(own=own, **dict(zip(BACKWARD, given)), **dict(zip(BACKWARD_SCRATCH, buffers))))
    for n, piece in enumerate(pieces):
        if n in BESIDE:
            rest.go(BESIDE.index(n))
        piece()
    rest.go(rest.last)


BESIDE = (0, 3, NSETS, STRIPES, SUB, 9)


def backward_call(given, left):
    tokens, d = given[0].shape
    whole = pl.BlockSpec(memory_space=pltpu.VMEM)
    blocks = [(FFN_WAVES, k, SUB, LANES) for _, _, k in SETS] + [(OWN_WAVES, devices(), k, SUB, LANES) for _, _, k in SETS]
    return pl.pallas_call(
        backward_kernel,
        out_shape=[jax.ShapeDtypeStruct(s, BF16) for s in blocks],
        in_specs=[whole] * (len(given) + NSETS),
        out_specs=[whole] * 12,
        scratch_shapes=backward_scratch(tokens, d) + late_buffers(FFN_WAVES),
        compiler_params=pltpu.CompilerParams(collective_id=PAIR, has_side_effects=True, vmem_limit_bytes=room(*left)),
        cost_estimate=pl.CostEstimate(flops=18_000_000_000, transcendentals=4_000_000, bytes_accessed=25_000_000),
    )(*given, *in_vmem(left))


def rotation(tokens):
    half = HEAD // PAIR
    pace = THETA ** (-jnp.arange(half, dtype=F32) / half)
    angles = [jnp.arange(*places, dtype=F32)[:, None] * pace for places in ((0, tokens, 32), (32,))]
    return [jnp.stack([jnp.cos(angle), jnp.sin(angle)]) for angle in angles]


def solution(mesh):
    def step(x, dy, *arrays):
        n = len(NAMES)
        w, m, v = (arrays[n * i : n * i + n] for i in range(3))
        wq, wk, wv, wo, gate, up, down = w
        x, dy = x[0], dy[0]
        a, q, k, value, out, lse, h, b, *turns = forward_call(x, wq, wk, wv, wo, *rotation(x.shape[0]))
        left, (by_b,) = deal(ffn_call(b, dy, gate, up, down), NSETS)
        shares, own = deal(backward_call((dy, h, by_b, a, q, k, value, out, lse, wo, *turns), left), NSETS)
        gs, (total, *ahead) = deal(gather_call(shares, own, [(m, v)[kind][n] for kind, n in AHEAD]), NSETS)
        return tuple(adam_call(w, m, v, total, gs, ahead))

    states, all_of = P(("rep", "dp"), None, None), P(None, None, None)
    return jax.shard_map(
        step,
        mesh=mesh,
        in_specs=(states, states) + (all_of,) * 21,
        out_specs=(P("rep", None, None),) * 21,
        check_vma=False,
    )
```

```python
import functools
import math

import jax
import jax.numpy as jnp
from jax import lax
from jax.experimental import pallas as pl
from jax.experimental.pallas import tpu as pltpu
from jax.sharding import PartitionSpec as P

THETA = 10000
NAMES = ("wq", "wk", "wv", "wo", "w_gate", "w_up", "w_down")
PAIR = 2
LANES = 128
STRIPES = 7
NSETS = 6
SUB = 8
TILE = 16
HALF_PART = 64
F32, BF16 = jnp.float32, jnp.bfloat16
VM = 66_000_000


def room(*arrays):
    return VM - sum(math.prod(a.shape) * jnp.dtype(a.dtype).itemsize for a in arrays)
DIMS = {"x": 4, "y": 4, "z": SUB}
ORDER = {"A": ("x", "y", "z"), "B": ("y", "x", "z"), "C": ("z", "x", "y")}
SETS = (("A", -1, PAIR), ("A", 1, PAIR), ("B", -1, PAIR), ("B", 1, PAIR), ("C", -1, PAIR), ("C", 1, 1))
WAVE = tuple((c, 0) for c in range(NSETS)) + ((4, 1),) + tuple((c, 1) for c in range(4))


def vm(shape, dtype):
    return pltpu.VMEM(shape, dtype)


def in_vmem(arrays):
    return [pltpu.with_memory_space_constraint(a, pltpu.VMEM) for a in arrays]


def deal(refs, *counts):
    got = []
    for count in counts:
        got.append(refs[:count])
        refs = refs[count:]
    return (*got, refs)


def sizes(cls):
    return tuple(DIMS[d] for d in ORDER[cls])


def devices():
    return math.prod(DIMS.values())


class Place:
    def __init__(self):
        i = lax.axis_index("dp")
        ny, nz = DIMS["y"], DIMS["z"]
        self.at = {"x": i // (ny * nz), "y": (i // nz) % ny, "z": i % nz}
        self.places = {(d, far): (self.at[d] + far) % n if far else self.at[d] for d, n in DIMS.items() for far in range(n)}
        self.peers = {}
        for d, far in self.places:
            at = {**self.at, d: self.places[d, far]}
            self.peers[d, far] = {"dp": (at["x"] * ny + at["y"]) * nz + at["z"]}

    def beside(self, d, far):
        return self.peers[d, far % DIMS[d]]

    def block(self, d, far):
        return self.places[d, far % DIMS[d]]

    def slot(self, cls):
        d1, d2, d3 = ORDER[cls]
        return (self.at[d1] * DIMS[d2] + self.at[d2]) * DIMS[d3] + self.at[d3]


def greet(peers):
    barrier = pltpu.get_barrier_semaphore()
    for peer in peers:
        pl.semaphore_signal(barrier, inc=1, device_id=peer)
    pl.semaphore_wait(barrier, len(peers))


def line_peers(me):
    return [me.beside(d, s) for d, n in DIMS.items() for s in range(1, n)]


def chain(n):
    half = n // PAIR
    stages = []
    for i in range(1, half + 1):
        far = half - i + 1
        now = [(1, far, None if i == 1 else i - PAIR, i - 1)]
        if i >= PAIR:
            now.append((-1, far, None if i == PAIR else half + i - 3, half + i - PAIR))
        stages.append(now)
    return stages, [half - 1] + ([n - PAIR] if half >= PAIR else [])


def arrived(ref, sem):
    pltpu.make_async_copy(ref, ref, sem).wait()


class Reduce:
    def __init__(self, me, d, sign, own_at, send_at, recv_at, size, sent, came, step, raw):
        self.me, self.d, self.sign, self.n = me, d, sign, DIMS[d]
        self.own_at, self.send_at, self.recv_at = own_at, send_at, recv_at
        self.size, self.sent, self.came, self.step, self.raw = size, sent, came, min(step, size), raw
        self.stages, self.last = chain(self.n)

    def each(self, body):
        if self.size == self.step:
            body(0)
        else:
            lax.fori_loop(0, self.size // self.step, lambda i, _: body(i * self.step), None)

    def go(self, stage):
        if stage > 0:
            arrived(self.recv_at(0, 0, self.size, len(self.stages[stage - 1])), self.came(stage - 1))
        if stage == len(self.stages):
            return
        for way, far, joins, into in self.stages[stage]:
            block = self.me.block(self.d, self.sign * way * far)
            if joins is not None or not self.raw:
                def body(first):
                    v = self.own_at(block, first, self.step)[...].astype(F32)
                    if joins is not None:
                        v = v + self.recv_at(joins, first, self.step, 1)[0].astype(F32)
                    self.send_at(block, first, self.step)[...] = v.astype(BF16)
                self.each(body)
            pltpu.make_async_remote_copy(self.send_at(block, 0, self.size), self.recv_at(into, 0, self.size, 1).at[0], self.sent, self.came(stage),
                                         device_id=self.me.beside(self.d, self.sign * way)).start()

    def finish(self, put):
        def body(first):
            v = self.own_at(self.me.at[self.d], first, self.step)[...].astype(F32)
            for r in self.last:
                v = v + self.recv_at(r, first, self.step, 1)[0].astype(F32)
            put(first, self.step, v)
        self.each(body)

    def drain(self):
        arrived(self.send_at(0, 0, self.size * (self.n - 1)), self.sent)


class DirectReduce:
    stages = (None,)

    def __init__(self, me, d, own_at, send_at, recv_at, sent, came):
        self.me, self.d, self.n = me, d, DIMS[d]
        self.own_at, self.send_at, self.recv_at, self.sent, self.came = own_at, send_at, recv_at, sent, came

    def go(self, stage):
        if stage == 1:
            arrived(self.recv_at(0, 0, 1, self.n - 1), self.came(0))
            return
        for far in range(1, self.n):
            block = self.send_at(self.me.block(self.d, far), 0, 1)
            block[...] = self.own_at(self.me.block(self.d, far), 0, 1)[...].astype(BF16)
            pltpu.make_async_remote_copy(block, self.recv_at(far - 1, 0, 1, 1).at[0], self.sent, self.came(0), device_id=self.me.beside(self.d, far)).start()

    def finish(self, put):
        v = self.own_at(self.me.at[self.d], 0, 1)[...].astype(F32)
        for far in range(self.n - 1):
            v = v + self.recv_at(far, 0, 1, 1)[0].astype(F32)
        put(0, 1, v)

    def drain(self):
        arrived(self.send_at(0, 0, self.n - 1), self.sent)


class Gather:
    def __init__(self, me, d, sign, at, sent, came):
        self.me, self.d, self.sign, self.n, self.at, self.sent, self.came = me, d, sign, DIMS[d], at, sent, came
        half = self.n // PAIR
        self.stages = [[way for way in (1, -1) if stage < half or way == sign] for stage in range(1, half + 1)]

    def go(self, stage):
        if stage > 0:
            arrived(self.at(0, len(self.stages[stage - 1])), self.came(stage - 1))
        if stage < len(self.stages):
            for way in self.stages[stage]:
                block = self.at(self.me.block(self.d, -way * stage), 1)
                pltpu.make_async_remote_copy(block, block, self.sent, self.came(stage), device_id=self.me.beside(self.d, way)).start()

    def drain(self):
        arrived(self.at(0, self.n - 1), self.sent)


class DirectGather:
    stages = (None,)

    def __init__(self, me, d, at, sent, came):
        self.me, self.d, self.n, self.at, self.sent, self.came = me, d, DIMS[d], at, sent, came

    def go(self, stage):
        if stage == 1:
            arrived(self.at(0, self.n - 1), self.came(0))
            return
        block = self.at(self.me.at[self.d], 1)
        for far in range(1, self.n):
            pltpu.make_async_remote_copy(block, block, self.sent, self.came(0), device_id=self.me.beside(self.d, far)).start()

    def drain(self):
        arrived(self.at(0, self.n - 1), self.sent)


class GroupSum:
    def __init__(self, me, ref, sent, came):
        self.me, self.ref, self.sent, self.came = me, ref, sent, came
        self.names = list(DIMS)

    def ring(self, n):
        return DirectGather(self.me, self.names[n], lambda i, many: self.ref.at[n, pl.ds(i, many)], self.sent.at[n], lambda stage: self.came.at[n])

    def go(self, n):
        if n > 0:
            before = self.ring(n - 1)
            before.go(1)
            total = self.ref[n - 1, 0]
            for i in range(1, before.n):
                total = total + self.ref[n - 1, i]
            to = self.me.at[self.names[n]] if n < len(self.names) else 0
            self.ref[n, pl.ds(to, 1)] = total[None]
            before.drain()
        if n < len(self.names):
            self.ring(n).go(0)


STAGES = 4


class Reduction:
    def __init__(self, me, tb, rx, left, sent, came):
        self.me, self.tb, self.rx, self.left, self.sent, self.came = me, tb, rx, left, sent, came

    def step(self, wave, slot, event):
        for c, (cls, sign, _) in enumerate(SETS):
            n1, n2, n3 = sizes(cls)
            size = n2 * n3
            pace = 4 // (n1 // PAIR)
            if event % pace == 0:
                own = lambda block, first, step: self.tb[c].at[slot, pl.ds(block * size + first, step)]
                ring = Reduce(self.me, ORDER[cls][0], sign, own, own, lambda i, first, step, many: self.rx[c].at[wave, pl.ds(i, many), pl.ds(first, step)], size,
                              self.sent.at[wave, c], lambda stage: self.came.at[wave, c, stage], SUB, True)
                ring.go(event // pace)
                if event == 4:
                    def put(first, step, v):
                        self.left[c][wave, pl.ds(first, step)] = v
                    ring.finish(put)
                    ring.drain()


class Late:
    def __init__(self, me, left, refs, put, direct):
        send2, rx2, acc3, send3, rx3, (sent, came) = deal(refs, NSETS, NSETS, NSETS, NSETS, NSETS)
        self.acc3, self.put, self.rings = acc3, put, []
        for c, (cls, sign, _) in enumerate(SETS):
            self.rings.append(self.of(me, cls, sign, left[c], send2[c], rx2[c], acc3[c], send3[c], rx3[c], sent.at[0, c], sent.at[1, c],
                                      functools.partial(lambda c, ring, stage: came.at[ring, c, stage], c), direct))
        self.last = max(len(two.stages) + len(three.stages) for two, three in self.rings)

    @staticmethod
    def of(me, cls, sign, left, send2, rx2, acc3, send3, rx3, sent2, sent3, came, direct):
        _, d2, d3 = ORDER[cls]
        n3 = DIMS[d3]
        two = Reduce(me, d2, sign, lambda b, f, st: left.at[:, pl.ds(b * n3 + f, st)], lambda b, f, st: send2.at[:, pl.ds(b * n3 + f, st)],
                     lambda i, f, st, many: rx2.at[pl.ds(i, many), :, pl.ds(f, st)], n3, sent2, functools.partial(came, 0), 4, False)
        at3 = (lambda b, f, st: acc3.at[:, pl.ds(b + f, st)], lambda b, f, st: send3.at[:, pl.ds(b + f, st)], lambda i, f, st, many: rx3.at[pl.ds(i, many)])
        if direct:
            return two, DirectReduce(me, d3, *at3, sent3, functools.partial(came, 1))
        return two, Reduce(me, d3, sign, *at3, 1, sent3, functools.partial(came, 1), 1, False)

    def go(self, event):
        for c, (two, three) in enumerate(self.rings):
            half = len(two.stages)
            if event <= half:
                two.go(event)
            if event == half:
                def put3(first, step, v):
                    self.acc3[c][:, pl.ds(first, step)] = v
                two.finish(put3)
            if half <= event <= half + len(three.stages):
                three.go(event - half)
            if event == half + len(three.stages):
                three.finish(lambda first, step, v: self.put(c, v[:, 0]))
                two.drain()
                three.drain()


def late_buffers(waves):
    made = [[] for _ in range(5)]
    for cls, _, k in SETS:
        n1, n2, n3 = sizes(cls)
        for to, shape, dtype in zip(made, ((waves, n2 * n3), (n2 - 1, waves, n3), (waves, n3), (waves, n3), (n3 - 1, waves, 1)), (BF16, BF16, F32, BF16, BF16)):
            to.append(vm((*shape, k, SUB, LANES), dtype))
    return sum(made, []) + light_sems()


def semaphores(*shapes):
    return [pltpu.SemaphoreType.DMA(shape) for shape in shapes]


def reduction_buffers(slots, waves):
    tb, rx = [], []
    for cls, _, k in SETS:
        n1, n2, n3 = sizes(cls)
        tb.append(vm((slots, devices(), k, SUB, LANES), BF16))
        rx.append(vm((waves, n1 - 1, n2 * n3, k, SUB, LANES), BF16))
    return [*tb, *rx, *semaphores((waves, NSETS), (waves, NSETS, STAGES))]


class LightGather:
    def __init__(self, me, at, sent, came, direct):
        self.rings = [self.of(me, cls, sign, functools.partial(at, c), sent.at[0, c], sent.at[1, c],
                              functools.partial(lambda c, ring, stage: came.at[ring, c, stage], c), direct) for c, (cls, sign, _) in enumerate(SETS)]
        self.last = max(len(three.stages) + len(two.stages) for three, two in self.rings)

    @staticmethod
    def of(me, cls, sign, at, sent2, sent3, came, direct):
        _, d2, d3 = ORDER[cls]
        n3 = DIMS[d3]
        at3 = lambda i, many: at(me.at[d2] * n3 + i, many)
        if direct:
            three = DirectGather(me, d3, at3, sent3, functools.partial(came, 1))
        else:
            three = Gather(me, d3, sign, at3, sent3, functools.partial(came, 1))
        return three, Gather(me, d2, sign, lambda i, many: at(i * n3, many * n3), sent2, functools.partial(came, 0))

    def go(self, event):
        for three, two in self.rings:
            first = len(three.stages)
            if event <= first:
                three.go(event)
            if first <= event <= first + len(two.stages):
                two.go(event - first)
            if event == first + len(two.stages):
                three.drain()
                two.drain()


def light_sems():
    return semaphores((PAIR, NSETS), (PAIR, NSETS, STAGES))


FFN_WAVES, OWN_WAVES = STRIPES, PAIR
HALVES = ((0, 4), (4, 3))
BEHIND = PAIR


def left_shapes():
    return [(FFN_WAVES, sizes(cls)[1] * sizes(cls)[PAIR], k, SUB, LANES) for cls, _, k in SETS]


def reduce_loop(waves, reduction, slots, pieces):
    def body(i, _):
        for p, piece in enumerate(pieces):
            for event in reversed(range(5)):
                back = p - PAIR - PAIR * event
                if back % len(pieces) == 0:
                    w = i + back // len(pieces)

                    @pl.when((w >= 0) & (w < waves))
                    def _():
                        reduction.step(w, w % slots, event)

            @pl.when(i < waves)
            def _():
                piece(i)

    lax.fori_loop(0, waves + 3, body, None)


FF_CHUNK = 512
TOKEN_BLOCK = 512


def ffn_kernel(waves, x_ref, dy_ref, wg_ref, wu_ref, wd_ref, *refs):
    left, (db_ref, *refs) = deal(refs, NSETS)
    tb, rx, (sent, came, *rest) = deal(refs, NSETS, NSETS)
    wbuf, wdbuf, hid_s, dg_s, du_s, dbg, dbu, wsem = rest
    me = Place()
    slots = tb[0].shape[0]

    def weights(j, s):
        cols = pl.ds(pl.multiple_of(j * FF_CHUNK, FF_CHUNK), FF_CHUNK)
        return [pltpu.make_async_copy(wg_ref.at[0, :, cols], wbuf.at[s, 0], wsem.at[s, 0]),
                pltpu.make_async_copy(wu_ref.at[0, :, cols], wbuf.at[s, 1], wsem.at[s, 1]),
                pltpu.make_async_copy(wd_ref.at[0, cols, :], wdbuf.at[s], wsem.at[s, PAIR])]

    for copy in weights(0, 0):
        copy.start()
    dbg[...] = jnp.zeros_like(dbg)
    dbu[...] = jnp.zeros_like(dbu)
    pad_c, pad_k = WAVE[10]
    for s in range(slots):
        tb[pad_c][s, devices() // PAIR:, pad_k] = jnp.zeros((devices() // PAIR, SUB, LANES), BF16)
    greet(line_peers(me))

    def hidden_units(j):
        s = j % PAIR
        for copy in weights(j, s):
            copy.wait()

        @pl.when(j + 1 < waves)
        def _():
            for copy in weights(j + 1, 1 - s):
                copy.start()

        def tokens(n, _):
            rows = pl.ds(pl.multiple_of(n * TOKEN_BLOCK, TOKEN_BLOCK), TOKEN_BLOCK)
            b = x_ref[rows, :]
            gate = _dot(b, wbuf[s, 0], 1, 0)
            up = _dot(b, wbuf[s, 1], 1, 0)
            dh = _dot(dy_ref[rows, :], wdbuf[s], 1, 1).astype(BF16).astype(F32)
            sig = 1.0 / (1.0 + jnp.exp(-gate))
            silu = gate * sig
            hid_s[rows, :] = (silu * up).astype(BF16)
            du_s[rows, :] = (dh * silu).astype(BF16)
            dg_s[rows, :] = (dh * up * (sig + silu * (1.0 - sig))).astype(BF16)

        lax.fori_loop(0, x_ref.shape[0] // TOKEN_BLOCK, tokens, None)

    def by_weights(j):
        slot = j % slots
        for half, src in enumerate((dg_s, du_s)):
            g = _dot(x_ref[...], src[...], 0, 0).astype(BF16)
            for t in range(STRIPES):
                c, k = WAVE[t]
                for i in range(4):
                    tb[c][slot, pl.ds(HALF_PART * half + TILE * i, TILE), k] = g[LANES * t : LANES * t + LANES, LANES * i : LANES * i + LANES].reshape(TILE, SUB, LANES)
        g = _dot(hid_s[...], dy_ref[...], 0, 0).astype(BF16)
        for i in range(STRIPES):
            c, k = WAVE[STRIPES + i // PAIR]
            tb[c][slot, pl.ds(HALF_PART * (i % PAIR), HALF_PART), k] = g[:, LANES * i : LANES * i + LANES].reshape(HALF_PART, SUB, LANES)

    def by_input(j):
        for n, (to, src) in enumerate(((dbg, dg_s), (dbu, du_s))):
            to[...] += _dot(src[...], wbuf[j % PAIR, n], 1, 1)

    reduce_loop(waves, Reduction(me, tb, rx, left, sent, came), slots, (hidden_units, by_weights, by_input))
    db_ref[...] = (dbg[...].astype(BF16).astype(F32) + dbu[...].astype(BF16).astype(F32)).astype(BF16)


def ffn_call(b, dy, wg, wu, wd):
    waves = wg.shape[PAIR] // FF_CHUNK
    tokens, d = b.shape
    whole = pl.BlockSpec(memory_space=pltpu.VMEM)
    anywhere = pl.BlockSpec(memory_space=pl.ANY)
    mid = vm((tokens, FF_CHUNK), BF16)
    left = [vm(s, F32) for s in left_shapes()]
    return pl.pallas_call(
        functools.partial(ffn_kernel, waves),
        out_shape=left + [vm((tokens, d), BF16)],
        in_specs=[whole, whole, anywhere, anywhere, anywhere],
        out_specs=[whole] * STRIPES,
        scratch_shapes=reduction_buffers(3, waves) + [
            vm((PAIR, PAIR, d, FF_CHUNK), BF16), vm((PAIR, FF_CHUNK, d), BF16), mid, mid, mid, vm((tokens, d), F32), vm((tokens, d), F32),
            pltpu.SemaphoreType.DMA((PAIR, 3))],
        compiler_params=pltpu.CompilerParams(collective_id=0, has_side_effects=True, vmem_limit_bytes=room(b, b, *left)),
        cost_estimate=pl.CostEstimate(flops=TILE * tokens * d * wg.shape[PAIR], transcendentals=tokens * wg.shape[PAIR], bytes_accessed=40_000_000),
    )(*in_vmem([b]), dy, wg, wu, wd)


def share_slot(me, cls):
    d1, d2, d3 = ORDER[cls]
    return me.at[d2] * DIMS[d3] + me.at[d3]


def gather_kernel(*refs):
    shares, tb_in, moments, g, (tot_out, *refs) = deal(refs, NSETS, NSETS, len(AHEAD), NSETS)
    ahead, refs = deal(refs, len(AHEAD))
    tb, rx, left, (sent, came, *refs) = deal(refs, NSETS, NSETS, NSETS)
    late, (nrm, lsem, msem, ns, nr, g1s, g1r, *light) = deal(refs, len(refs) - 13)
    me = Place()
    waves = FFN_WAVES + OWN_WAVES

    loads = [pltpu.make_async_copy(tb_in[c], tb[c], lsem.at[c]) for c in range(NSETS)]
    fetched = [pltpu.make_async_copy(src, to, msem.at[n]) for n, (src, to) in enumerate(zip(moments, ahead))]
    for copy in loads + fetched:
        copy.start()
    for c, (cls, _, _) in enumerate(SETS):
        g[c][:FFN_WAVES, me.slot(cls)] = shares[c][...]
    greet(line_peers(me))
    for copy in loads:
        copy.wait()

    def put(c, v):
        g[c][FFN_WAVES:, me.slot(SETS[c][0])] = v.astype(BF16)

    def block(first_wave, count):
        def at(c, first, size):
            cls, _, _ = SETS[c]
            _, n2, n3 = sizes(cls)
            return g[c].at[pl.ds(first_wave, count), pl.ds(me.at[ORDER[cls][0]] * n2 * n3 + first, size)]
        return at

    reduction = Reduction(me, tb, rx, left, sent, came)
    rest = Late(me, left, late, put, True)
    summing = GroupSum(me, nrm, ns, nr)
    spread_ffn = [LightGather(me, block(*half), *light[PAIR * n : PAIR * n + PAIR], False) for n, half in enumerate(HALVES)]
    spread = LightGather(me, block(FFN_WAVES, OWN_WAVES), *light[-PAIR:], True)

    def norm():
        total = jnp.zeros((SUB, LANES), F32)
        for c, (cls, _, _) in enumerate(SETS):
            v = g[c][:, me.slot(cls)].astype(F32)
            total = total + jnp.sum(v * v, axis=(0, 1))
        nrm[0, pl.ds(me.at["x"], 1)] = total[None]

    ready = 4 + rest.last

    def chain(point):
        if point < 5:
            for w in range(OWN_WAVES):
                reduction.step(w, w, point)
        for n, half in enumerate(spread_ffn):
            if 0 <= point - BEHIND * n <= half.last:
                half.go(point - BEHIND * n)
        if 4 <= point <= ready:
            rest.go(point - 4)
        if point == ready:
            norm()
        if ready <= point <= ready + max(spread.last, len(DIMS)):
            if point - ready <= spread.last:
                spread.go(point - ready)
            if point - ready <= len(DIMS):
                summing.go(point - ready)

    def far(wave, event):
        for c, (cls, sign, _) in enumerate(SETS):
            n1, n2, n3 = sizes(cls)
            pace = 4 // (n1 // PAIR)
            if event % pace == 0:
                size = n2 * n3
                ring = Gather(me, ORDER[cls][0], sign, lambda i, many: g[c].at[wave, pl.ds(i * size, many * size)], g1s.at[wave, c],
                              lambda stage: g1r.at[wave, c, stage])
                ring.go(event // pace)
                if event == 4:
                    ring.drain()

    begin = spread_ffn[0].last // PAIR

    def body(i, _):
        for half in range(PAIR):
            for point in range(half, ready + 1 + max(spread.last, len(DIMS)), PAIR):
                @pl.when(i == point // PAIR)
                def _():
                    chain(point)
            for event in reversed(range(half, 5, PAIR)):
                w = i - event - begin

                @pl.when((w >= 0) & (w < waves))
                def _():
                    far(w, event)

    lax.fori_loop(0, waves + 4 + begin, body, None)
    tot_out[...] = nrm[len(DIMS), 0]
    for copy in fetched:
        copy.wait()


AHEAD = tuple((kind, n) for n in range(4) for kind in range(PAIR))


def gather_call(shares, own, moments):
    waves = FFN_WAVES + OWN_WAVES
    whole = pl.BlockSpec(memory_space=pltpu.VMEM)
    anywhere = pl.BlockSpec(memory_space=pl.ANY)
    left = [vm((OWN_WAVES, *s[1:]), F32) for s in left_shapes()]
    buffers, sems = deal(reduction_buffers(OWN_WAVES, OWN_WAVES), 12)
    kept = [vm((waves, devices(), k, SUB, LANES), BF16) for _, _, k in SETS] + [vm((SUB, LANES), F32)] + [vm(a.shape, F32) for a in moments]
    return pl.pallas_call(
        gather_kernel,
        out_shape=kept,
        in_specs=[whole] * NSETS + [anywhere] * (NSETS + len(moments)),
        out_specs=[whole] * (STRIPES + len(moments)),
        scratch_shapes=buffers + left + sems + late_buffers(OWN_WAVES) + [vm((4, SUB, SUB, LANES), F32)]
        + semaphores((NSETS,), (len(moments),), (len(DIMS),), (len(DIMS),), (waves, NSETS), (waves, NSETS, STAGES)) + light_sems() * (1 + len(HALVES)),
        compiler_params=pltpu.CompilerParams(collective_id=1, has_side_effects=True, vmem_limit_bytes=room(*kept)),
        cost_estimate=pl.CostEstimate(flops=10_000_000_000, transcendentals=0, bytes_accessed=60_000_000),
    )(*shares, *own, *moments)


COUNT = 12386304


def attention_parts():
    return [(kind, t) for kind in ("o", "kv", "q") for t in range(STRIPES)]


def place_of(kind, j, t):
    if kind in ("gu", "d"):
        c, k = WAVE[t if kind == "gu" else STRIPES + t]
        return c, j, k
    n = attention_parts().index((kind, t))
    c, k = WAVE[n % 11]
    return c, FFN_WAVES + n // 11, k


def adam_job(kind, j, n):
    if kind in ("gu", "q", "kv"):
        rows = LANES * n
        col = pl.multiple_of(512 * j, 512) if kind == "gu" else 0
        pieces = {"gu": [(4, rows, col, 512, 0), (5, rows, col, 512, 512)], "q": [(0, rows, 0, 1024, 0)], "kv": [(1, rows, 0, 512, 0), (PAIR, rows, 0, 512, 512)]}
        return pieces[kind], [(*place_of(kind, j, n), TILE * i) for i in range(SUB)]
    if kind == "o":
        return [(3, LANES * n, 0, 896, 0)], [(*place_of(kind, j, t), TILE * n) for t in range(STRIPES)]
    row = pl.multiple_of(512 * j + LANES * n, LANES)
    return [(NSETS, row, 0, 896, 0)], [(*place_of(kind, j, t // PAIR), HALF_PART * (t % PAIR) + TILE * n) for t in range(STRIPES)]


ROUND = [("gu", n) for n in range(STRIPES)] + [("d", n) for n in range(4)]
REST = [("o", n) for n in range(SUB)] + [(kind, n) for kind in ("kv", "q") for n in range(STRIPES)]


def adam_kernel(depth, *refs):
    n = len(NAMES)
    w, m, v, (tot, *refs) = deal(refs, n, n, n)
    g, held, wo, mo, vo, rest = deal(refs, NSETS, len(AHEAD), n, n, n)
    wb, mb, vb, wn, mn, vn, isem, osem = rest
    ahead, period = depth - 1, len(ROUND)

    def moves(job, s, out):
        made = []
        for n, (which, row, col, width, at) in enumerate(job[0]):
            for a, (old, new, near, late) in enumerate(((w, wo, wb, wn), (m, mo, mb, mn), (v, vo, vb, vn))):
                if not out and (a - 1, which) in AHEAD:
                    continue
                far = (new if out else old)[which].at[0, pl.ds(row, LANES), pl.ds(col, width)]
                here = (late if out else near).at[s, :, pl.ds(at, width)]
                made.append(pltpu.make_async_copy(here, far, osem.at[s, n, a]) if out else pltpu.make_async_copy(far, here, isem.at[s, n, a]))
        return made

    def start(job, s, out):
        for copy in moves(job, s, out):
            copy.start()

    def finish(job, s, out):
        for copy in moves(job, s, out):
            copy.wait()

    def work(job, s):
        def body(r, _):
            rows = pl.ds(pl.multiple_of(TILE * r, TILE), TILE)

            def moment(kind, n, buf):
                which, row, _, width, at = [p for p in job[0] if p[4] <= LANES * n][-1]
                if (kind, which) in AHEAD:
                    return held[AHEAD.index((kind, which))][0, pl.ds(pl.multiple_of(row + TILE * r, TILE), TILE), LANES * n - at : LANES * n - at + LANES]
                return buf[s, rows, LANES * n : LANES * n + LANES]

            for n, (c, wave, k, slot) in enumerate(job[1]):
                cols = slice(LANES * n, LANES * n + LANES)
                x = g[c][wave, pl.ds(slot + PAIR * r, PAIR), k].astype(F32).reshape(TILE, LANES) * factor
                a = 0.9 * moment(0, n, mb) + 0.1 * x
                b = 0.95 * moment(1, n, vb) + 0.05 * x * x
                old = wb[s, rows, cols].astype(F32)
                mn[s, rows, cols] = a
                vn[s, rows, cols] = b
                wn[s, rows, cols] = (old - 0.02 * (a * lax.rsqrt(b + 1e-8) + 0.1 * old)).astype(BF16)

        lax.fori_loop(0, SUB, body, None)

    for i in range(ahead):
        start(adam_job(*(ROUND[i][0], 0, ROUND[i][1])), i, False)
    square = jnp.sum(tot[...], keepdims=True)
    factor = jnp.broadcast_to(jnp.minimum(1.0, 0.5 * lax.rsqrt(square / COUNT + 1e-30)), (TILE, LANES))
    job_of = lambda i, j: adam_job(ROUND[i][0], j, ROUND[i][1])
    rest_job = lambda i: adam_job(REST[i][0], 0, REST[i][1])

    def chunk(j, _):
        for i in range(period):
            at = period * j + i
            s = lax.rem(at, depth)
            nxt = lax.rem(at + ahead, depth)
            if i + ahead < period:
                start(job_of(i + ahead, j), nxt, False)
            else:
                later = i + ahead - period

                @pl.when(j + 1 < FFN_WAVES)
                def _():
                    start(job_of(later, j + 1), nxt, False)

                @pl.when(j + 1 == FFN_WAVES)
                def _():
                    start(rest_job(later), nxt, False)
            finish(job_of(i, j), s, False)
            if i >= depth:
                finish(job_of(i - depth, j), s, True)
            else:
                @pl.when(j > 0)
                def _():
                    finish(job_of(i - depth + period, j - 1), s, True)
            work(job_of(i, j), s)
            start(job_of(i, j), s, True)

    lax.fori_loop(0, FFN_WAVES, chunk, None)
    base = period * FFN_WAVES
    for i in range(len(REST)):
        s = (base + i) % depth
        if i + ahead < len(REST):
            start(rest_job(i + ahead), (base + i + ahead) % depth, False)
        finish(rest_job(i), s, False)
        finish(rest_job(i - depth) if i >= depth else job_of(i - depth + period, FFN_WAVES - 1), s, True)
        work(rest_job(i), s)
        start(rest_job(i), s, True)
    for i in range(len(REST) - depth, len(REST)):
        finish(rest_job(i), (base + i) % depth, True)


def adam_call(w, m, v, tot, gs, ahead, depth=4):
    anywhere = pl.BlockSpec(memory_space=pl.ANY)
    whole = pl.BlockSpec(memory_space=pltpu.VMEM)
    buf = lambda t: vm((depth, LANES, 1024), t)
    dma = pltpu.SemaphoreType.DMA
    return pl.pallas_call(
        functools.partial(adam_kernel, depth),
        out_shape=[jax.ShapeDtypeStruct(x.shape, x.dtype) for x in (*w, *m, *v)],
        in_specs=[anywhere] * 21 + [whole] * (STRIPES + len(ahead)),
        out_specs=[anywhere] * 21,
        scratch_shapes=[buf(BF16), buf(F32), buf(F32)] * PAIR + [dma((depth, PAIR, 3))] * PAIR,
        compiler_params=pltpu.CompilerParams(vmem_limit_bytes=room(tot, *gs, *ahead)),
        cost_estimate=pl.CostEstimate(flops=25 * COUNT, transcendentals=COUNT, bytes_accessed=270_000_000),
    )(*w, *m, *v, *in_vmem([tot, *gs, *ahead]))


HEAD, GROUPS, PER = 256, PAIR, PAIR
QB = 256
LOG2E = 1.4426950408889634


def _dot(a, b, ca, cb):
    return lax.dot_general(a, b, (((ca,), (cb,)), ((), ())), preferred_element_type=F32)


def root(wide):
    return lax.rsqrt(jnp.mean(wide * wide, -1, keepdims=True) + 1e-6)


def turn(t, cos, sin):
    a, b = t[:, : HEAD // PAIR], t[:, HEAD // PAIR :]
    return jnp.concatenate([a * cos - b * sin, b * cos + a * sin], -1)


def head(g, h):
    return pl.ds(pl.multiple_of((PER * g + h) * HEAD, HEAD), HEAD)


def stacked(ref, rows, g):
    return jnp.concatenate([ref[rows, head(g, h)] for h in range(PER)], 0)


def hidden(s, fill):
    n = s.shape[0]
    own = s[n - QB :]
    key = lax.broadcasted_iota(jnp.int32, own.shape, 0)
    query = lax.broadcasted_iota(jnp.int32, own.shape, 1) % QB
    own = jnp.where(key <= query, own, fill)
    return own if n == QB else jnp.concatenate([s[: n - QB], own], 0)


def forward_kernel(x, wq, wk, wv, wo_far, far, near, *refs):
    b_o, outs, made, (wo, sem) = refs[0], *deal(refs[1:], 9, 9)
    a_o, q_o, k_o, v_o, out_o, lse_o, h_o, cos, sin = made
    fetch = pltpu.make_async_copy(wo_far, wo, sem.at[9])
    fetch.start()
    leave = [pltpu.make_async_copy(src, to, sem.at[n]) for n, (src, to) in enumerate(zip(made, outs))]
    tokens = x.shape[0]
    big = 512
    some = near.shape[1]

    def angles(n, _):
        rows = pl.ds(pl.multiple_of(n * some, some), some)
        c, s = far[0, pl.ds(n, 1)], far[1, pl.ds(n, 1)]
        cos[rows, :] = c * near[0] - s * near[1]
        sin[rows, :] = s * near[0] + c * near[1]

    lax.fori_loop(0, tokens // some, angles, None)

    def project(n, _):
        rows = pl.ds(pl.multiple_of(n * big, big), big)
        wide = x[rows, :].astype(F32)
        a = (wide * root(wide)).astype(BF16)
        a_o[rows, :] = a
        c, s = cos[rows, :], sin[rows, :]
        for w, to in ((wq, q_o), (wk, k_o)):
            t = _dot(a, w[0], 1, 0).astype(BF16).astype(F32)
            for at in range(0, t.shape[1], HEAD):
                to[rows, at : at + HEAD] = turn(t[:, at : at + HEAD], c, s).astype(BF16)
        v_o[rows, :] = _dot(a, wv[0], 1, 0).astype(BF16)

    lax.fori_loop(0, tokens // big, project, None)
    for n in (0, 1, PAIR, 3, STRIPES, SUB):
        leave[n].start()
    e = HEAD**-0.5 * LOG2E

    def attend(g, _):
        cols = pl.ds(pl.multiple_of(g * HEAD, HEAD), HEAD)
        for i in range(tokens // QB):
            rows, n = slice(QB * i, QB * i + QB), QB * (i + 1)
            s = hidden(_dot(k_o[:n, cols], stacked(q_o, rows, g), 1, 1), -1e30)
            top = s.max(0, keepdims=True)
            p = jnp.exp2((s - top) * e)
            total = p.sum(0, keepdims=True)
            p = (p * (1.0 / total)).astype(BF16)
            out = _dot(v_o[:n, cols], p, 0, 0).T.astype(BF16)
            lse = top * e + jnp.log2(total)
            for h in range(PER):
                out_o[rows, head(g, h)] = out[QB * h : QB * h + QB]
                lse_o[g, h : h + 1, rows] = lse[:, QB * h : QB * h + QB]

    lax.fori_loop(0, GROUPS, attend, None)
    for n in (4, 5):
        leave[n].start()
    fetch.wait()

    def finish(n, _):
        rows = pl.ds(pl.multiple_of(n * big, big), big)
        h = (x[rows, :].astype(F32) + _dot(out_o[rows, :], wo[0], 1, 0).astype(BF16).astype(F32)).astype(BF16)
        h_o[rows, :] = h
        wide = h.astype(F32)
        b_o[rows, :] = (wide * root(wide)).astype(BF16)

    lax.fori_loop(0, tokens // big, finish, None)
    leave[NSETS].start()
    for copy in leave:
        copy.wait()


def forward_call(x, wq, wk, wv, wo, far, near):
    tokens, d = x.shape
    nq, nk = wq.shape[PAIR], wk.shape[PAIR]
    shapes = [((tokens, n), BF16) for n in (d, nq, nk, nk, nq)] + [((GROUPS, PER, tokens), F32), ((tokens, d), BF16)] + [((tokens, HEAD // PAIR), F32)] * PAIR
    whole = pl.BlockSpec(memory_space=pltpu.VMEM)
    anywhere = pl.BlockSpec(memory_space=pl.ANY)
    b = vm((tokens, d), BF16)
    return pl.pallas_call(
        forward_kernel,
        out_shape=[b] + [jax.ShapeDtypeStruct(*s) for s in shapes],
        in_specs=[whole] * 4 + [anywhere] + [whole] * PAIR,
        out_specs=[whole] + [anywhere] * len(shapes),
        scratch_shapes=[vm(*s) for s in shapes] + [vm(wo.shape, BF16)] + semaphores((len(shapes) + 1,)),
        compiler_params=pltpu.CompilerParams(vmem_limit_bytes=room(b)),
        cost_estimate=pl.CostEstimate(flops=12_000_000_000, transcendentals=4_000_000, bytes_accessed=25_000_000),
    )(x, wq, wk, wv, wo, far, near)


def own_place(kind, t):
    c, wave, k = place_of(kind, 0, t)
    return c, wave - FFN_WAVES, k


def backward_pieces(refs):
    r = refs
    tokens = r.dy.shape[0]
    big = 512
    e, scale = HEAD**-0.5 * LOG2E, HEAD**-0.5

    def by_norm():
        def body(n, _):
            rows = pl.ds(pl.multiple_of(n * big, big), big)
            wide = r.h[rows, :].astype(F32)
            by = r.by_b[rows, :].astype(F32)
            s = root(wide)
            back = by * s - wide * (s * s * s * jnp.mean(by * wide, -1, keepdims=True))
            r.by_h[rows, :] = (r.dy[rows, :].astype(F32) + back.astype(BF16).astype(F32)).astype(BF16)
            r.by_out[rows, :] = _dot(r.by_h[rows, :], r.wo[0], 1, 1).astype(BF16)

        lax.fori_loop(0, tokens // big, body, None)

    def by_wo():
        g = _dot(r.out[...], r.by_h[...], 0, 0).astype(BF16)
        for t in range(STRIPES):
            c, w, k = own_place("o", t)
            r.own[c][w, :, k] = g[:, LANES * t : LANES * t + LANES].reshape(devices(), SUB, LANES)

    def attend(i):
        rows, n = slice(QB * i, QB * i + QB), QB * (i + 1)

        def body(g, _):
            cols = pl.ds(pl.multiple_of(g * HEAD, HEAD), HEAD)
            q, do = stacked(r.q, rows, g), stacked(r.by_out, rows, g)
            lse = jnp.concatenate([r.lse[g, h : h + 1, rows] for h in range(PER)], 1)
            p = hidden(jnp.exp2(_dot(r.k[:n, cols], q, 1, 1) * e - lse), 0.0)
            dp = _dot(r.v[:n, cols], do, 1, 1)
            delta = (p * dp).sum(0, keepdims=True)
            ds = (p * (dp - delta)).astype(BF16)
            r.by_v[:n, cols] += _dot(p.astype(BF16), do, 1, 0)
            r.by_k[:n, cols] += _dot(ds, q, 1, 0)
            dq = (_dot(r.k[:n, cols], ds, 0, 0) * scale).T.astype(BF16).astype(F32)
            for h in range(PER):
                r.by_q[rows, head(g, h)] = turn(dq[QB * h : QB * h + QB], r.cos[rows, :], -r.sin[rows, :]).astype(BF16)

        return lambda: lax.fori_loop(0, GROUPS, body, None)

    def clear():
        r.by_k[...] = jnp.zeros_like(r.by_k)
        r.by_v[...] = jnp.zeros_like(r.by_v)

    def by_w(kind, first, source):
        g = _dot(r.a[...], source, 0, 0).astype(BF16)
        for t in range(STRIPES):
            c, w, k = own_place(kind, t)
            for n in range(4):
                r.own[c][w, pl.ds(TILE * (first + n), TILE), k] = g[LANES * t : LANES * t + LANES, LANES * n : LANES * n + LANES].reshape(TILE, SUB, LANES)

    def by_keys():
        by_w("kv", 0, jnp.concatenate([turn((r.by_k[:, HEAD * g : HEAD * g + HEAD] * scale).astype(BF16).astype(F32), r.cos[...], -r.sin[...]).astype(BF16)
                                       for g in range(GROUPS)], 1))

    def by_queries():
        lax.fori_loop(0, PAIR, lambda n, _: by_w("q", 4 * n, r.by_q[:, pl.ds(pl.multiple_of(512 * n, 512), 512)]), None)

    return [clear, by_norm, by_wo, *(attend(i) for i in range(tokens // QB)), lambda: by_w("kv", 4, r.by_v[...].astype(BF16)), by_keys, by_queries]


class Names:
    def __init__(self, **refs):
        self.__dict__.update(refs)


BACKWARD = ("dy", "h", "wo", "out", "q", "k", "v", "lse", "cos", "sin", "a")
NEEDED = {1: 3, PAIR: 4, 3: 10, STRIPES: 11}
BACKWARD_SCRATCH = ("by_h", "by_out", "by_q", "by_k", "by_v")


def backward_scratch(tokens, d):
    wide, key = GROUPS * PER * HEAD, GROUPS * HEAD
    return [vm((tokens, d), BF16), vm((tokens, wide), BF16), vm((tokens, wide), BF16), vm((tokens, key), F32), vm((tokens, key), F32)]


def backward_kernel(*refs):
    by_b, given, left, shares, own, refs = refs[0], *deal(refs[1:], len(BACKWARD), NSETS, NSETS, NSETS)
    buffers, here, (sem, *refs) = deal(refs, len(BACKWARD_SCRATCH), len(BACKWARD))
    fetch = [pltpu.make_async_copy(src, to, sem.at[n]) for n, (src, to) in enumerate(zip(given, here))]
    for copy in fetch:
        copy.start()
    me = Place()

    def put(c, v):
        shares[c][...] = v.astype(BF16)

    pad, k = WAVE[10]
    own[pad][OWN_WAVES - 1, :, k] = jnp.zeros((devices(), SUB, LANES), BF16)
    greet(line_peers(me))
    rest = Late(me, left, refs, put, False)
    pieces = backward_pieces(Names(own=own, by_b=by_b, **dict(zip(BACKWARD, here)), **dict(zip(BACKWARD_SCRATCH, buffers))))
    had = 0
    for n, piece in enumerate(pieces):
        for copy in fetch[had : NEEDED.get(n, had)]:
            copy.wait()
        had = NEEDED.get(n, had)
        if n in BESIDE:
            rest.go(BESIDE.index(n))
        piece()
    rest.go(rest.last)


BESIDE = (0, 3, NSETS, STRIPES, SUB, 9)


def backward_call(by_b, given, left):
    tokens, d = by_b.shape
    anywhere = pl.BlockSpec(memory_space=pl.ANY)
    whole = pl.BlockSpec(memory_space=pltpu.VMEM)
    blocks = [(FFN_WAVES, k, SUB, LANES) for _, _, k in SETS] + [(OWN_WAVES, devices(), k, SUB, LANES) for _, _, k in SETS]
    return pl.pallas_call(
        backward_kernel,
        out_shape=[jax.ShapeDtypeStruct(s, BF16) for s in blocks],
        in_specs=[whole] + [anywhere] * len(given) + [whole] * NSETS,
        out_specs=[whole] * 12,
        scratch_shapes=backward_scratch(tokens, d) + [vm(a.shape, a.dtype) for a in given] + semaphores((len(given),)) + late_buffers(FFN_WAVES),
        compiler_params=pltpu.CompilerParams(collective_id=PAIR, has_side_effects=True, vmem_limit_bytes=room(by_b, *left)),
        cost_estimate=pl.CostEstimate(flops=18_000_000_000, transcendentals=4_000_000, bytes_accessed=25_000_000),
    )(*in_vmem([by_b]), *given, *in_vmem(left))


def rotation(tokens):
    half = HEAD // PAIR
    pace = THETA ** (-jnp.arange(half, dtype=F32) / half)
    angles = [jnp.arange(*places, dtype=F32)[:, None] * pace for places in ((0, tokens, 32), (32,))]
    return [jnp.stack([jnp.cos(angle), jnp.sin(angle)]) for angle in angles]


def solution(mesh):
    def step(x, dy, *arrays):
        n = len(NAMES)
        w, m, v = (arrays[n * i : n * i + n] for i in range(3))
        wq, wk, wv, wo, gate, up, down = w
        x, dy = x[0], dy[0]
        b, a, q, k, value, out, lse, h, *turns = forward_call(x, wq, wk, wv, wo, *rotation(x.shape[0]))
        left, (by_b,) = deal(ffn_call(b, dy, gate, up, down), NSETS)
        shares, own = deal(backward_call(by_b, (dy, h, wo, out, q, k, value, lse, *turns, a), left), NSETS)
        gs, (total, *ahead) = deal(gather_call(shares, own, [(m, v)[kind][n] for kind, n in AHEAD]), NSETS)
        return tuple(adam_call(w, m, v, total, gs, ahead))

    states, all_of = P(("rep", "dp"), None, None), P(None, None, None)
    return jax.shard_map(
        step,
        mesh=mesh,
        in_specs=(states, states) + (all_of,) * 21,
        out_specs=(P("rep", None, None),) * 21,
        check_vma=False,
    )
```
